128 devices in a mesh: batch: 1, row: 16 (over z, y), col: 8 (over x, core).
Axes of the slice: x: 4, y: 4, z: 4, core: 2. Of those that a mesh axis runs over, the one named last changes fastest.
Arguments:
- lower_mat: bfloat16 [16384, 16384], P('row', 'col')
- rhs_mat: bfloat16 [16384, 2048], P('row', ('batch', 'col'))
Outputs:
- output: bfloat16 [16384, 2048], P('row', ('batch', 'col'))
All inputs are finite; a program needn't handle non-finite values.
Results may differ from the reference program's by a relative error of at most 0.001.
Values are sent between devices in bfloat16 or wider.
A program may use at most 1 GiB of HBM per device.

```python
import jax
import jax.numpy as jnp
from jax import lax

MAT_ORDER = 16384
BLOCK_SIZE = 256
RHS_COLS = 2048
GRID_ROWS = 16
GRID_COLS = 8


def stored_to_global(positions, grid_size):
    per_device = MAT_ORDER // grid_size
    device_idx = positions // per_device
    local_pos = positions % per_device
    return ((local_pos // BLOCK_SIZE) * grid_size + device_idx) * BLOCK_SIZE + local_pos % BLOCK_SIZE


def setup_inputs(seed: int = 0, part: int = 0) -> dict:
    key_mat, key_rhs = jax.random.split(jax.random.key(seed))
    col_global = stored_to_global(jnp.arange(MAT_ORDER), GRID_COLS)

    def draw_rows(block_idx):
        row_global = stored_to_global(block_idx * BLOCK_SIZE + jnp.arange(BLOCK_SIZE), GRID_ROWS)
        draws = jax.random.normal(jax.random.fold_in(key_mat, block_idx), (BLOCK_SIZE, MAT_ORDER), jnp.float32)
        scaled = draws / jnp.sqrt((row_global + 1).astype(jnp.float32))[:, None]
        keep = col_global[None, :] <= row_global[:, None]
        return jnp.where(keep, scaled, 0.0).astype(jnp.bfloat16)

    lower_mat = lax.map(draw_rows, jnp.arange(MAT_ORDER // BLOCK_SIZE)).reshape(MAT_ORDER, MAT_ORDER)
    rhs_mat = jax.random.normal(jax.random.fold_in(key_rhs, part), (MAT_ORDER, RHS_COLS), jnp.float32).astype(jnp.bfloat16)
    return {"lower_mat": lower_mat, "rhs_mat": rhs_mat}


def reference(lower_mat, rhs_mat):
    total_blocks = MAT_ORDER // BLOCK_SIZE
    row_blocks = total_blocks // GRID_ROWS
    col_blocks = total_blocks // GRID_COLS
    rhs_global = rhs_mat.reshape(GRID_ROWS, row_blocks, BLOCK_SIZE, RHS_COLS).transpose(1, 0, 2, 3).reshape(MAT_ORDER, RHS_COLS)
    outputs = []
    for stored_block in range(total_blocks):
        global_block = (stored_block % row_blocks) * GRID_ROWS + stored_block // row_blocks
        width = (global_block + 1) * BLOCK_SIZE
        row_panel = lower_mat[stored_block * BLOCK_SIZE:(stored_block + 1) * BLOCK_SIZE]
        panel_global = row_panel.reshape(BLOCK_SIZE, GRID_COLS, col_blocks, BLOCK_SIZE).transpose(0, 2, 1, 3).reshape(BLOCK_SIZE, MAT_ORDER)
        block_sum = jnp.dot(panel_global[:, :width], rhs_global[:width], preferred_element_type=jnp.float32)
        outputs.append(block_sum.astype(jnp.bfloat16))
    return jnp.concatenate(outputs, axis=0)
```

```python
import jax
import jax.numpy as jnp
from jax import lax
from jax.experimental import pallas as pl
from jax.experimental.pallas import tpu as pltpu
from jax.sharding import PartitionSpec as P

BLOCK = 256
HALF = 128
STAGES = 8
SLABS = 4
MESH = pl.DeviceIdType.MESH
F32 = jnp.float32


def _rem4(v):
    return lax.rem(v + 8, 4)


def _kernel(l_hbm, b_hbm, out_ref, l_all, b_all, acc, relay_lo, relay_hi, from_lo, from_hi,
            l_loc_sem, l_send_sem, l_recv_sem, b_send, b_recv, r_send, r_recv):
    row = lax.axis_index("row")
    col = lax.axis_index("col")
    z, y = row // 4, lax.rem(row, 4)
    x, core = col // 2, lax.rem(col, 2)

    def dev(zz, yy, xx, cc=None):
        return {"row": zz * 4 + yy, "col": xx * 2 + (core if cc is None else cc)}

    z_lo, z_hi = dev(_rem4(z - 1), y, x), dev(_rem4(z + 1), y, x)
    y_lo, y_hi = dev(z, _rem4(y - 1), x), dev(z, _rem4(y + 1), x)
    x_lo, x_hi = dev(z, y, _rem4(x - 1)), dev(z, y, _rem4(x + 1))
    partner = dev(z, y, x, 1 - core)

    def root_info(zt, yt):
        dz = _rem4(zt - x // 2)
        dy = _rem4(yt - 2 * lax.rem(x, 2) + 1)
        off_z, blk = lax.rem(dz, 2), dz // 2
        par, off_y = dy // 2, 1 - lax.rem((dy + 1) // 2, 2)
        return off_z, blk, par, off_y

    def unit(kind, zt, yt):
        off_z, blk, par, off_y = root_info(zt, yt)
        if kind == 0:
            return blk * 256 + par * HALF, (2 * off_z + off_y) * HALF
        return 512 + par * 256 + blk * HALF, (2 * off_y + off_z) * HALF

    def region(kind, zt, yt):
        off_z, blk, par, off_y = root_info(zt, yt)
        if kind == 0:
            return blk * 256, off_z * 256
        return 512 + par * 256, off_y * 256

    tgt_x = 2 * lax.rem(z, 2) + y // 2
    own_par = lax.rem(y, 2)

    def target(kind):
        hi, lo = x // 2, lax.rem(x, 2)
        off_z, off_y = (hi, lo) if kind == 0 else (lo, hi)
        return _rem4(z + off_z), _rem4(y + (2 * own_par - 1) * off_y)

    def source(kind):
        off_z, blk, par, off_y = root_info(z, y)
        xs = 2 * off_z + off_y if kind == 0 else 2 * off_y + off_z
        return dev(x // 2 + 2 * blk, 2 * lax.rem(x, 2) + par, xs)

    targets = [target(0), target(1)]
    to_self = [jnp.logical_and(jnp.logical_and(zt == z, yt == y), tgt_x == x) for zt, yt in targets]

    def slab_cols(ab, blk, par):
        return ab * 512 + (blk * 256 + par * HALF if ab == 0 else par * 256 + blk * HALF)

    def slab_copies(s):
        for ab in range(2):
            for blk in range(2):
                src = l_hbm.at[pl.ds(s * BLOCK, 1024 - s * BLOCK), pl.ds((2 * s + blk) * BLOCK + ab * HALF, HALF)]
                step = 256 if ab else HALF
                dst_col = pl.multiple_of(slab_cols(ab, blk, 0) + core * step, HALF)
                dst = l_all.at[s, pl.ds(s * BLOCK, 1024 - s * BLOCK), pl.ds(dst_col, HALF)]
                yield 2 * ab + blk, src, dst

    for s in range(SLABS):
        for i, src, dst in slab_copies(s):
            pltpu.make_async_copy(src, dst, l_loc_sem.at[s, i]).start()

    barrier = pltpu.get_barrier_semaphore()
    for d in (z_lo, z_hi, y_lo, y_hi, x_lo, x_hi, partner, source(0), source(1)):
        pl.semaphore_signal(barrier, inc=1, device_id=d, device_id_type=MESH)
    pl.semaphore_wait(barrier, 9)

    sends = []

    def send(src, dst, s_sem, r_sem, where):
        cp = pltpu.make_async_remote_copy(src_ref=src, dst_ref=dst, send_sem=s_sem, recv_sem=r_sem,
                                          device_id=where, device_id_type=MESH)
        cp.start()
        sends.append(cp)

    def arrived(ref, sem):
        pltpu.make_async_copy(ref, ref, sem).wait()

    def home_piece(t, kind):
        s, h = t // 2, t % 2
        src = b_hbm.at[pl.ds(s * BLOCK + kind * HALF, HALF), pl.ds(h * HALF, HALF)]
        blk, par = z // 2, own_par
        r0 = blk * 256 + par * HALF if kind == 0 else 512 + par * 256 + blk * HALF
        dst = b_all.at[t, pl.ds(pl.multiple_of(r0, HALF), HALF), pl.ds(pl.multiple_of(x * HALF, HALF), HALF)]
        return src, dst

    def root_copy(t, kind):
        src, dst = home_piece(t, kind)
        zt, yt = targets[kind]
        return pltpu.make_async_remote_copy(src_ref=src, dst_ref=dst, send_sem=b_send.at[t, kind], recv_sem=b_recv.at[t, kind],
                                            device_id=dev(zt, yt, tgt_x), device_id_type=MESH)

    for kind in range(2):
        @pl.when(jnp.logical_not(to_self[kind]))
        def _():
            for t in range(STAGES):
                root_copy(t, kind).start()

        @pl.when(to_self[kind])
        def _():
            for t in range(STAGES):
                src, dst = home_piece(t, kind)
                pltpu.make_async_copy(src, dst, b_recv.at[t, kind]).start()

    for s in range(SLABS):
        for i, src, dst in slab_copies(s):
            send(src, dst, l_send_sem.at[s, i], l_recv_sem.at[s, i], partner)

    def unit_ref(t, kind, zt, yt):
        r0, c0 = unit(kind, zt, yt)
        return b_all.at[t, pl.ds(pl.multiple_of(r0, HALF), HALF), pl.ds(pl.multiple_of(c0, HALF), HALF)]

    def region_ref(t, kind, zt, yt):
        r0, c0 = region(kind, zt, yt)
        return b_all.at[t, pl.ds(pl.multiple_of(r0, 256), 256), pl.ds(pl.multiple_of(c0, 256), 256)]

    lo_pos = [(z, _rem4(y - 1)), (_rem4(z - 1), y)]
    hi_pos = [(z, _rem4(y + 1)), (_rem4(z + 1), y)]
    lo_dev, hi_dev = [y_lo, z_lo], [y_hi, z_hi]
    any_unit = b_all.at[0, pl.ds(0, HALF), pl.ds(0, HALF)]
    any_region = b_all.at[0, pl.ds(0, 256), pl.ds(0, 256)]

    def gather_own(t, kind, phase):
        axis = kind if phase == 0 else 1 - kind
        ref = unit_ref(t, kind, z, y) if phase == 0 else region_ref(t, kind, z, y)
        base = 2 + 6 * kind + 3 * phase
        send(ref, ref, b_send.at[t, base], b_recv.at[t, base], hi_dev[axis])
        send(ref, ref, b_send.at[t, base + 1], b_recv.at[t, base + 1], lo_dev[axis])

    def gather_relay(t, kind, phase):
        axis = kind if phase == 0 else 1 - kind
        up = (t + kind + phase) % 2 == 0
        pos = lo_pos[axis] if up else hi_pos[axis]
        base = 2 + 6 * kind + 3 * phase
        arrived(any_unit if phase == 0 else any_region, b_recv.at[t, base if up else base + 1])
        ref = unit_ref(t, kind, *pos) if phase == 0 else region_ref(t, kind, *pos)
        send(ref, ref, b_send.at[t, base + 2], b_recv.at[t, base + 2], hi_dev[axis] if up else lo_dev[axis])

    def gather_rest(t, kind, phase):
        up = (t + kind + phase) % 2 == 0
        base = 2 + 6 * kind + 3 * phase
        ref = any_unit if phase == 0 else any_region
        arrived(ref, b_recv.at[t, base + 1 if up else base])
        arrived(ref, b_recv.at[t, base + 2])

    def first_own(t):
        for kind in range(2):
            arrived(any_unit, b_recv.at[t, kind])
            gather_own(t, kind, 0)

    def first_relay(t):
        for kind in range(2):
            gather_relay(t, kind, 0)

    def second_own(t):
        for kind in range(2):
            gather_rest(t, kind, 0)
            gather_own(t, kind, 1)

    def second_relay(t):
        for kind in range(2):
            gather_relay(t, kind, 1)

    def product(t, sp):
        s, h = t // 2, t % 2
        lhs = l_all[s, sp * BLOCK:(sp + 1) * BLOCK, :]
        for n in range(2):
            p = jnp.dot(lhs, b_all[t, :, n * 256:(n + 1) * 256], preferred_element_type=F32)
            for j in range(2):
                part = p[:, j * HALF:(j + 1) * HALF]
                if s > 0:
                    part = part + acc[sp, h, 2 * n + j]
                acc[sp, h, 2 * n + j] = part

    def compute(t):
        s = t // 2
        for kind in range(2):
            gather_rest(t, kind, 1)
        if t % 2 == 0:
            for i in range(4):
                arrived(l_all.at[s, pl.ds(s * BLOCK, 1024 - s * BLOCK), pl.ds(0, HALF)], l_loc_sem.at[s, i])
                arrived(l_all.at[s, pl.ds(s * BLOCK, 1024 - s * BLOCK), pl.ds(0, HALF)], l_recv_sem.at[s, i])
        product(t, s)

    def part_ref(t, slot, half):
        return acc.at[t // 2, t % 2, slot, pl.ds(half * HALF, HALF), :]

    xp1, xm1, xp2 = _rem4(x + 1), _rem4(x - 1), _rem4(x + 2)

    def reduce_first(t):
        send(part_ref(t, xp2, 0), relay_lo.at[t], r_send.at[t, 0], r_recv.at[t, 0], x_hi)
        send(part_ref(t, xp2, 1), relay_hi.at[t], r_send.at[t, 1], r_recv.at[t, 1], x_lo)
        send(part_ref(t, xp1, 1), from_lo.at[t, pl.ds(HALF, HALF), :], r_send.at[t, 2], r_recv.at[t, 2], x_hi)
        send(part_ref(t, xm1, 0), from_hi.at[t, pl.ds(0, HALF), :], r_send.at[t, 3], r_recv.at[t, 3], x_lo)

    def reduce_second(t):
        s, h = t // 2, t % 2
        arrived(relay_lo.at[t], r_recv.at[t, 0])
        acc[s, h, xp1, 0:HALF, :] = acc[s, h, xp1, 0:HALF, :] + relay_lo[t]
        send(part_ref(t, xp1, 0), from_lo.at[t, pl.ds(0, HALF), :], r_send.at[t, 4], r_recv.at[t, 4], x_hi)
        arrived(relay_hi.at[t], r_recv.at[t, 1])
        acc[s, h, xm1, HALF:BLOCK, :] = acc[s, h, xm1, HALF:BLOCK, :] + relay_hi[t]
        send(part_ref(t, xm1, 1), from_hi.at[t, pl.ds(HALF, HALF), :], r_send.at[t, 5], r_recv.at[t, 5], x_lo)

    def finish(t):
        s, h = t // 2, t % 2
        for i in (2, 3, 4, 5):
            arrived(relay_lo.at[t], r_recv.at[t, i])
        total = acc[s, h, x] + from_lo[t] + from_hi[t]
        out_ref[s * BLOCK:(s + 1) * BLOCK, h * HALF:(h + 1) * HALF] = total.astype(out_ref.dtype)

    for i in range(STAGES + 6):
        if i < STAGES:
            first_own(i)
        if 0 <= i - 1 < STAGES:
            first_relay(i - 1)
        if 0 <= i - 2 < STAGES:
            second_own(i - 2)
        if 0 <= i - 3 < STAGES:
            second_relay(i - 3)
        if 0 <= i - 4 < STAGES:
            compute(i - 4)
            reduce_first(i - 4)
        if 0 <= i - 5 < STAGES:
            reduce_second(i - 5)
        if 0 <= i - 4 < STAGES:
            for sp in range((i - 4) // 2 + 1, SLABS):
                product(i - 4, sp)
        if 0 <= i - 6 < STAGES:
            finish(i - 6)

    for cp in sends:
        cp.wait_send()
    for kind in range(2):
        @pl.when(jnp.logical_not(to_self[kind]))
        def _():
            for t in range(STAGES):
                root_copy(t, kind).wait_send()


def solution(mesh):
    def local_product(lower_loc, rhs_loc):
        rows, cols = rhs_loc.shape
        bf16 = lower_loc.dtype
        return pl.pallas_call(
            _kernel,
            out_shape=jax.ShapeDtypeStruct((rows, cols), bf16),
            in_specs=[pl.BlockSpec(memory_space=pl.ANY)] * 2,
            out_specs=pl.BlockSpec(memory_space=pltpu.VMEM),
            scratch_shapes=[
                pltpu.VMEM((SLABS, 1024, 1024), bf16),
                pltpu.VMEM((STAGES, 1024, 512), bf16),
                pltpu.VMEM((SLABS, 2, 4, BLOCK, HALF), F32),
                pltpu.VMEM((STAGES, HALF, HALF), F32),
                pltpu.VMEM((STAGES, HALF, HALF), F32),
                pltpu.VMEM((STAGES, BLOCK, HALF), F32),
                pltpu.VMEM((STAGES, BLOCK, HALF), F32),
                pltpu.SemaphoreType.DMA((SLABS, 4)),
                pltpu.SemaphoreType.DMA((SLABS, 4)),
                pltpu.SemaphoreType.DMA((SLABS, 4)),
                pltpu.SemaphoreType.DMA((STAGES, 14)),
                pltpu.SemaphoreType.DMA((STAGES, 14)),
                pltpu.SemaphoreType.DMA((STAGES, 6)),
                pltpu.SemaphoreType.DMA((STAGES, 6)),
            ],
            compiler_params=pltpu.CompilerParams(collective_id=0, has_side_effects=True, vmem_limit_bytes=48 * 1024 * 1024),
        )(lower_loc, rhs_loc)

    return jax.shard_map(local_product, mesh=mesh, in_specs=(P("row", "col"), P("row", ("batch", "col"))), out_specs=P("row", ("batch", "col")), check_vma=False)
```

```python
import jax
import jax.numpy as jnp
from jax import lax
from jax.experimental import pallas as pl
from jax.experimental.pallas import tpu as pltpu
from jax.sharding import PartitionSpec as P

BLOCK = 256
HALF = 128
STAGES = 8
SLABS = 4
MESH = pl.DeviceIdType.MESH
F32 = jnp.float32
MOVE_FIRST = 2
ORDER = (("move", -2), ("enter", -1), ("own1", 0), ("relay1", 1), ("own2", 2), ("relay2", 3), ("compute", 4), ("reduce1", 4),
         ("reduce2", 5), ("others", 4), ("finish", 6))


def _rem4(v):
    return lax.rem(v + 8, 4)


def _kernel(l_hbm, b_hbm, out_ref, l_all, b_all, acc, relay_lo, relay_hi, from_lo, from_hi,
            l_loc_sem, l_send_sem, l_recv_sem, b_send, b_recv, r_send, r_recv, staged, m_send, m_recv):
    row = lax.axis_index("row")
    col = lax.axis_index("col")
    z, y = row // 4, lax.rem(row, 4)
    x, core = col // 2, lax.rem(col, 2)

    def dev(zz, yy, xx, cc=None):
        return {"row": zz * 4 + yy, "col": xx * 2 + (core if cc is None else cc)}

    z_lo, z_hi = dev(_rem4(z - 1), y, x), dev(_rem4(z + 1), y, x)
    y_lo, y_hi = dev(z, _rem4(y - 1), x), dev(z, _rem4(y + 1), x)
    x_lo, x_hi = dev(z, y, _rem4(x - 1)), dev(z, y, _rem4(x + 1))
    partner = dev(z, y, x, 1 - core)

    def offsets(kind, h, xs):
        v = 3 - xs if h else xs
        hi, lo = v // 2, lax.rem(v, 2)
        return (hi, lo) if kind == 0 else (lo, hi)

    def moved(kind, back, zz, yy, off_z, off_y):
        dz = off_z if (kind == 0) != back else -off_z
        return _rem4(zz + dz), _rem4(yy + (2 * lax.rem(yy, 2) - 1) * off_y)

    def plane_of(zz, yy):
        return 2 * lax.rem(zz, 2) + yy // 2

    def root_info(kind, zt, yt):
        dz = _rem4(zt - x // 2)
        dy = _rem4(yt - 2 * lax.rem(x, 2) + 1)
        off_z = lax.rem(dz, 2)
        blk = dz // 2 if kind == 0 else lax.rem((dz + 1) // 2, 2)
        par, off_y = dy // 2, 1 - lax.rem((dy + 1) // 2, 2)
        return off_z, blk, par, off_y

    def slab_copy(s):
        rows = pl.ds(s * BLOCK, 1024 - s * BLOCK)
        return l_hbm.at[rows, pl.ds(s * 512, 512)], l_all.at[s, rows, pl.ds(pl.multiple_of(core * 512, 512), 512)]

    for s in range(SLABS):
        src, dst = slab_copy(s)
        pltpu.make_async_copy(src, dst, l_loc_sem.at[s]).start()

    barrier = pltpu.get_barrier_semaphore()
    y_side = _rem4(y + 2 * lax.rem(y, 2) - 1)
    for d in (z_lo, z_hi, y_lo, y_hi, x_lo, x_hi, dev(z, y, _rem4(x + 2)), partner,
              dev(_rem4(z - 1), y_side, x), dev(_rem4(z + 1), y_side, x)):
        pl.semaphore_signal(barrier, inc=1, device_id=d, device_id_type=MESH)
    pl.semaphore_wait(barrier, 10)

    sends = []

    def send(src, dst, s_sem, r_sem, where):
        cp = pltpu.make_async_remote_copy(src_ref=src, dst_ref=dst, send_sem=s_sem, recv_sem=r_sem,
                                          device_id=where, device_id_type=MESH)
        cp.start()
        sends.append(cp)

    def arrived(ref, sem):
        pltpu.make_async_copy(ref, ref, sem).wait()

    in_plane = plane_of(z, y) == x

    def final_ref(t, kind, zs, ys, xs):
        return b_all.at[t, lax.rem(ys, 2), zs // 2, kind, :, pl.ds(pl.multiple_of(xs * HALF, HALF), HALF)]

    def move_copies(t, kind):
        s, h = t // 2, t % 2
        src = b_hbm.at[pl.ds(s * BLOCK + kind * HALF, HALF), pl.ds(h * HALF, HALF)]
        off_z, off_y = offsets(kind, h, x)
        zt, yt = moved(kind, False, z, y, off_z, off_y)
        stay = x == (3 if h else 0)
        for direct in (True, False):
            dst = final_ref(t, kind, z, y, x) if direct else staged.at[t, kind]
            sem = (b_recv if direct else m_recv).at[t, kind]
            cond = in_plane if direct else jnp.logical_not(in_plane)
            yield (jnp.logical_and(cond, stay), pltpu.make_async_copy(src, dst, sem), False)
            yield (jnp.logical_and(cond, jnp.logical_not(stay)),
                   pltpu.make_async_remote_copy(src_ref=src, dst_ref=dst, send_sem=m_send.at[t, kind], recv_sem=sem,
                                                device_id=dev(zt, yt, x), device_id_type=MESH), True)

    def move(t):
        for kind in range(2):
            for cond, cp, _ in move_copies(t, kind):
                pl.when(cond)(cp.start)

    def enter_copy(t, kind):
        off_z, off_y = offsets(kind, t % 2, x)
        zs, ys = moved(kind, True, z, y, off_z, off_y)
        xt = plane_of(zs, ys)
        cp = pltpu.make_async_remote_copy(src_ref=staged.at[t, kind], dst_ref=final_ref(t, kind, zs, ys, x),
                                          send_sem=b_send.at[t, kind], recv_sem=b_recv.at[t, kind],
                                          device_id=dev(z, y, xt), device_id_type=MESH)
        return xt != x, cp

    def enter(t):
        for kind in range(2):
            cond, cp = enter_copy(t, kind)

            @pl.when(cond)
            def _():
                arrived(staged.at[t, kind], m_recv.at[t, kind])
                cp.start()

    for t in range(MOVE_FIRST):
        move(t)

    for s in range(SLABS):
        src, dst = slab_copy(s)
        send(src, dst, l_send_sem.at[s], l_recv_sem.at[s], partner)

    def unit_ref(t, kind, zt, yt):
        off_z, blk, par, off_y = root_info(kind, zt, yt)
        v = 2 * off_z + off_y if kind == 0 else 2 * off_y + off_z
        xs = 3 - v if t % 2 else v
        return b_all.at[t, par, blk, kind, :, pl.ds(pl.multiple_of(xs * HALF, HALF), HALF)]

    def region_ref(t, kind, zt, yt):
        off_z, blk, par, off_y = root_info(kind, zt, yt)
        pair = off_z if kind == 0 else off_y
        cols = pl.ds(pl.multiple_of((1 - pair if t % 2 else pair) * 256, 256), 256)
        if kind == 0:
            return b_all.at[t, :, blk, 0, :, cols]
        return b_all.at[t, par, :, 1, :, cols]

    lo_pos = [(z, _rem4(y - 1)), (_rem4(z - 1), y)]
    hi_pos = [(z, _rem4(y + 1)), (_rem4(z + 1), y)]
    lo_dev, hi_dev = [y_lo, z_lo], [y_hi, z_hi]
    any_unit = b_all.at[0, 0, 0, 0, :, pl.ds(0, HALF)]
    any_region = b_all.at[0, 0, :, 0, :, pl.ds(0, 256)]

    def gather_own(t, kind, phase):
        axis = kind if phase == 0 else 1 - kind
        ref = unit_ref(t, kind, z, y) if phase == 0 else region_ref(t, kind, z, y)
        base = 2 + 6 * kind + 3 * phase
        send(ref, ref, b_send.at[t, base], b_recv.at[t, base], hi_dev[axis])
        send(ref, ref, b_send.at[t, base + 1], b_recv.at[t, base + 1], lo_dev[axis])

    def gather_relay(t, kind, phase):
        axis = kind if phase == 0 else 1 - kind
        up = (t + kind + phase) % 2 == 0
        pos = lo_pos[axis] if up else hi_pos[axis]
        base = 2 + 6 * kind + 3 * phase
        arrived(any_unit if phase == 0 else any_region, b_recv.at[t, base if up else base + 1])
        ref = unit_ref(t, kind, *pos) if phase == 0 else region_ref(t, kind, *pos)
        send(ref, ref, b_send.at[t, base + 2], b_recv.at[t, base + 2], hi_dev[axis] if up else lo_dev[axis])

    def gather_rest(t, kind, phase):
        up = (t + kind + phase) % 2 == 0
        base = 2 + 6 * kind + 3 * phase
        ref = any_unit if phase == 0 else any_region
        arrived(ref, b_recv.at[t, base + 1 if up else base])
        arrived(ref, b_recv.at[t, base + 2])

    def first_own(t):
        for kind in range(2):
            arrived(any_unit, b_recv.at[t, kind])
            gather_own(t, kind, 0)

    def first_relay(t):
        for kind in range(2):
            gather_relay(t, kind, 0)

    def second_own(t):
        for kind in range(2):
            gather_rest(t, kind, 0)
            gather_own(t, kind, 1)

    def second_relay(t):
        for kind in range(2):
            gather_relay(t, kind, 1)

    def product(t, sp):
        s, h = t // 2, t % 2
        lhs = l_all[s, sp * BLOCK:(sp + 1) * BLOCK, :]
        for n in range(2):
            rhs = b_all[t, :, :, :, :, n * 256:(n + 1) * 256].reshape(1024, 256)
            p = jnp.dot(lhs, rhs, preferred_element_type=F32)
            for j in range(2):
                part = p[:, j * HALF:(j + 1) * HALF]
                if s > 0:
                    part = part + acc[sp, h, 2 * n + j]
                acc[sp, h, 2 * n + j] = part

    def compute(t):
        s = t // 2
        for kind in range(2):
            gather_rest(t, kind, 1)
        if t % 2 == 0:
            for sem in (l_loc_sem, l_recv_sem):
                arrived(l_all.at[s, pl.ds(s * BLOCK, 1024 - s * BLOCK), pl.ds(0, 512)], sem.at[s])
        product(t, s)

    def part_ref(t, slot, half):
        return acc.at[t // 2, t % 2, slot, pl.ds(half * HALF, HALF), :]

    xp1, xm1, xp2 = _rem4(x + 1), _rem4(x - 1), _rem4(x + 2)

    def reduce_first(t):
        send(part_ref(t, xp2, 0), relay_lo.at[t], r_send.at[t, 0], r_recv.at[t, 0], x_hi)
        send(part_ref(t, xp2, 1), relay_hi.at[t], r_send.at[t, 1], r_recv.at[t, 1], x_lo)
        send(part_ref(t, xp1, 1), from_lo.at[t, pl.ds(HALF, HALF), :], r_send.at[t, 2], r_recv.at[t, 2], x_hi)
        send(part_ref(t, xm1, 0), from_hi.at[t, pl.ds(0, HALF), :], r_send.at[t, 3], r_recv.at[t, 3], x_lo)

    def reduce_second(t):
        s, h = t // 2, t % 2
        arrived(relay_lo.at[t], r_recv.at[t, 0])
        acc[s, h, xp1, 0:HALF, :] = acc[s, h, xp1, 0:HALF, :] + relay_lo[t]
        send(part_ref(t, xp1, 0), from_lo.at[t, pl.ds(0, HALF), :], r_send.at[t, 4], r_recv.at[t, 4], x_hi)
        arrived(relay_hi.at[t], r_recv.at[t, 1])
        acc[s, h, xm1, HALF:BLOCK, :] = acc[s, h, xm1, HALF:BLOCK, :] + relay_hi[t]
        send(part_ref(t, xm1, 1), from_hi.at[t, pl.ds(HALF, HALF), :], r_send.at[t, 5], r_recv.at[t, 5], x_lo)

    def finish(t):
        s, h = t // 2, t % 2
        for i in (2, 3, 4, 5):
            arrived(relay_lo.at[t], r_recv.at[t, i])
        total = acc[s, h, x] + from_lo[t] + from_hi[t]
        out_ref[s * BLOCK:(s + 1) * BLOCK, h * HALF:(h + 1) * HALF] = total.astype(out_ref.dtype)

    def others(t):
        for sp in range(t // 2 + 1, SLABS):
            product(t, sp)

    steps = {"move": move, "enter": enter, "own1": first_own, "relay1": first_relay, "own2": second_own, "relay2": second_relay,
             "compute": compute, "reduce1": reduce_first, "others": others, "reduce2": reduce_second, "finish": finish}
    for i in range(-4, STAGES + 8):
        for name, lag in ORDER:
            t = i - lag
            if 0 <= t < STAGES and not (name == "move" and t < MOVE_FIRST):
                steps[name](t)

    for cp in sends:
        cp.wait_send()
    for t in range(STAGES):
        for kind in range(2):
            for cond, cp, remote in move_copies(t, kind):
                if remote:
                    pl.when(cond)(cp.wait_send)
            cond, cp = enter_copy(t, kind)
            pl.when(cond)(cp.wait_send)


def solution(mesh):
    def local_product(lower_loc, rhs_loc):
        rows, cols = rhs_loc.shape
        bf16 = lower_loc.dtype
        return pl.pallas_call(
            _kernel,
            out_shape=jax.ShapeDtypeStruct((rows, cols), bf16),
            in_specs=[pl.BlockSpec(memory_space=pltpu.HBM)] * 2,
            out_specs=pl.BlockSpec(memory_space=pltpu.VMEM),
            scratch_shapes=[
                pltpu.VMEM((SLABS, 1024, 1024), bf16),
                pltpu.VMEM((STAGES, 2, 2, 2, HALF, 512), bf16),
                pltpu.VMEM((SLABS, 2, 4, BLOCK, HALF), F32),
                pltpu.VMEM((STAGES, HALF, HALF), F32),
                pltpu.VMEM((STAGES, HALF, HALF), F32),
                pltpu.VMEM((STAGES, BLOCK, HALF), F32),
                pltpu.VMEM((STAGES, BLOCK, HALF), F32),
                pltpu.SemaphoreType.DMA((SLABS,)),
                pltpu.SemaphoreType.DMA((SLABS,)),
                pltpu.SemaphoreType.DMA((SLABS,)),
                pltpu.SemaphoreType.DMA((STAGES, 14)),
                pltpu.SemaphoreType.DMA((STAGES, 14)),
                pltpu.SemaphoreType.DMA((STAGES, 6)),
                pltpu.SemaphoreType.DMA((STAGES, 6)),
                pltpu.VMEM((STAGES, 2, HALF, HALF), bf16),
                pltpu.SemaphoreType.DMA((STAGES, 2)),
                pltpu.SemaphoreType.DMA((STAGES, 2)),
            ],
            compiler_params=pltpu.CompilerParams(collective_id=0, has_side_effects=True, vmem_limit_bytes=63 * 1024 * 1024),
        )(lower_loc, rhs_loc)

    return jax.shard_map(local_product, mesh=mesh, in_specs=(P("row", "col"), P("row", ("batch", "col"))), out_specs=P("row", ("batch", "col")), check_vma=False)
```

```python
import jax
import jax.numpy as jnp
from jax import lax
from jax.experimental import pallas as pl
from jax.experimental.pallas import tpu as pltpu
from jax.sharding import PartitionSpec as P

BLOCK = 256
HALF = 128
STAGES = 8
SLABS = 4
MESH = pl.DeviceIdType.MESH
F32 = jnp.float32
MOVE_FIRST = 8
ORDER = (("move", -2), ("enter", -1), ("own1", 0), ("relay1", 1), ("own2", 2), ("relay2", 3), ("compute", 4), ("reduce1", 4),
         ("reduce2", 5), ("others", 4), ("finish", 7))


def _rem4(v):
    return lax.rem(v + 8, 4)


def _kernel(l_hbm, b_hbm, out_ref, l_all, b_all, acc, relay_lo, relay_hi, from_lo, from_hi,
            staged, l_recv, m_recv, b_recv, r_recv, sent):
    row = lax.axis_index("row")
    col = lax.axis_index("col")
    z, y = row // 4, lax.rem(row, 4)
    x, core = col // 2, lax.rem(col, 2)

    def dev(zz, yy, xx, cc=None):
        return {"row": zz * 4 + yy, "col": xx * 2 + (core if cc is None else cc)}

    z_lo, z_hi = dev(_rem4(z - 1), y, x), dev(_rem4(z + 1), y, x)
    y_lo, y_hi = dev(z, _rem4(y - 1), x), dev(z, _rem4(y + 1), x)
    x_lo, x_hi = dev(z, y, _rem4(x - 1)), dev(z, y, _rem4(x + 1))
    partner = dev(z, y, x, 1 - core)

    def offsets(kind, h, xs):
        v = 3 - xs if h else xs
        hi, lo = v // 2, lax.rem(v, 2)
        return (hi, lo) if kind == 0 else (lo, hi)

    def moved(kind, back, zz, yy, off_z, off_y):
        dz = off_z if (kind == 0) != back else -off_z
        return _rem4(zz + dz), _rem4(yy + (2 * lax.rem(yy, 2) - 1) * off_y)

    def plane_of(zz, yy):
        return 2 * lax.rem(zz, 2) + yy // 2

    def root_info(kind, zt, yt):
        dz = _rem4(zt - x // 2)
        dy = _rem4(yt - 2 * lax.rem(x, 2) + 1)
        off_z = lax.rem(dz, 2)
        blk = dz // 2 if kind == 0 else lax.rem((dz + 1) // 2, 2)
        par, off_y = dy // 2, 1 - lax.rem((dy + 1) // 2, 2)
        return off_z, blk, par, off_y

    def slab_copy(s):
        rows = pl.ds(s * BLOCK, 1024 - s * BLOCK)
        return l_hbm.at[rows, pl.ds(s * 512, 512)], l_all.at[s, rows, pl.ds(pl.multiple_of(core * 512, 512), 512)]

    for s in range(SLABS):
        src, dst = slab_copy(s)
        pltpu.make_async_copy(src, dst, l_recv.at[s]).start()

    barrier = pltpu.get_barrier_semaphore()
    y_side = _rem4(y + 2 * lax.rem(y, 2) - 1)
    for d in (z_lo, z_hi, y_lo, y_hi, x_lo, x_hi, dev(z, y, _rem4(x + 2)), partner,
              dev(_rem4(z - 1), y_side, x), dev(_rem4(z + 1), y_side, x)):
        pl.semaphore_signal(barrier, inc=1, device_id=d, device_id_type=MESH)
    pl.semaphore_wait(barrier, 10)

    def send(src, dst, s_sem, r_sem, where):
        cp = pltpu.make_async_remote_copy(src_ref=src, dst_ref=dst, send_sem=s_sem, recv_sem=r_sem,
                                          device_id=where, device_id_type=MESH)
        cp.start()

    def arrived(ref, sem):
        pltpu.make_async_copy(ref, ref, sem).wait()

    in_plane = plane_of(z, y) == x

    def final_ref(t, kind, zs, ys, xs):
        return b_all.at[t, lax.rem(ys, 2), zs // 2, kind, :, pl.ds(pl.multiple_of(xs * HALF, HALF), HALF)]

    def move_copies(t, kind):
        s, h = t // 2, t % 2
        src = b_hbm.at[pl.ds(s * BLOCK + kind * HALF, HALF), pl.ds(h * HALF, HALF)]
        off_z, off_y = offsets(kind, h, x)
        zt, yt = moved(kind, False, z, y, off_z, off_y)
        stay = x == (3 if h else 0)
        for direct in (True, False):
            dst = final_ref(t, kind, z, y, x) if direct else staged.at[t, kind]
            sem = b_recv.at[t, 0] if direct else m_recv.at[t, kind]
            cond = in_plane if direct else jnp.logical_not(in_plane)
            yield (jnp.logical_and(cond, stay), pltpu.make_async_copy(src, dst, sem), False)
            yield (jnp.logical_and(cond, jnp.logical_not(stay)),
                   pltpu.make_async_remote_copy(src_ref=src, dst_ref=dst, send_sem=sent.at[1], recv_sem=sem,
                                                device_id=dev(zt, yt, x), device_id_type=MESH), True)

    def move(t):
        for kind in range(2):
            for cond, cp, _ in move_copies(t, kind):
                pl.when(cond)(cp.start)

    def enter_copy(t, kind):
        off_z, off_y = offsets(kind, t % 2, x)
        zs, ys = moved(kind, True, z, y, off_z, off_y)
        xt = plane_of(zs, ys)
        cp = pltpu.make_async_remote_copy(src_ref=staged.at[t, kind], dst_ref=final_ref(t, kind, zs, ys, x),
                                          send_sem=sent.at[2], recv_sem=b_recv.at[t, 0],
                                          device_id=dev(z, y, xt), device_id_type=MESH)
        return xt != x, cp

    def enter(t):
        for kind in range(2):
            cond, cp = enter_copy(t, kind)

            @pl.when(cond)
            def _():
                arrived(staged.at[t, kind], m_recv.at[t, kind])
                cp.start()

    for t in range(MOVE_FIRST):
        move(t)

    for s in range(SLABS):
        src, dst = slab_copy(s)
        send(src, dst, sent.at[0], l_recv.at[s], partner)

    def unit_ref(t, kind, zt, yt):
        off_z, blk, par, off_y = root_info(kind, zt, yt)
        v = 2 * off_z + off_y if kind == 0 else 2 * off_y + off_z
        xs = 3 - v if t % 2 else v
        return b_all.at[t, par, blk, kind, :, pl.ds(pl.multiple_of(xs * HALF, HALF), HALF)]

    def region_ref(t, kind, zt, yt, half):
        off_z, blk, par, off_y = root_info(kind, zt, yt)
        pair = off_z if kind == 0 else off_y
        cols = pl.ds(pl.multiple_of((1 - pair if t % 2 else pair) * 256, 256), 256)
        if kind == 0:
            return b_all.at[t, half, blk, 0, :, cols]
        return b_all.at[t, par, half, 1, :, cols]

    lo_pos = [(z, _rem4(y - 1)), (_rem4(z - 1), y)]
    hi_pos = [(z, _rem4(y + 1)), (_rem4(z + 1), y)]
    lo_dev, hi_dev = [y_lo, z_lo], [y_hi, z_hi]
    any_unit = b_all.at[0, 0, 0, 0, :, pl.ds(0, HALF)]
    any_region = b_all.at[0, 0, 0, 0, :, pl.ds(0, 256)]

    def unit_own(t, kind):
        ref, up = unit_ref(t, kind, z, y), (t + kind) % 2 == 0
        send(ref, ref, sent.at[3], b_recv.at[t, 1 if up else 2], hi_dev[kind])
        send(ref, ref, sent.at[3], b_recv.at[t, 2 if up else 1], lo_dev[kind])

    def unit_relay(t, kind):
        up = (t + kind) % 2 == 0
        ref = unit_ref(t, kind, *(lo_pos if up else hi_pos)[kind])
        send(ref, ref, sent.at[3], b_recv.at[t, 2], (hi_dev if up else lo_dev)[kind])

    def region_own(t, kind):
        axis = 1 - kind
        for j in range(2):
            up, down = region_ref(t, kind, z, y, j), region_ref(t, kind, z, y, 1 - j)
            send(up, up, sent.at[4], b_recv.at[t, 7 if j else 3 + 2 * kind], hi_dev[axis])
            send(down, down, sent.at[4], b_recv.at[t, 7 if j else 4 + 2 * kind], lo_dev[axis])

    def region_relay(t, kind):
        axis = 1 - kind
        arrived(any_region, b_recv.at[t, 3 + 2 * kind])
        ref = region_ref(t, kind, *lo_pos[axis], 0)
        send(ref, ref, sent.at[4], b_recv.at[t, 7], hi_dev[axis])
        arrived(any_region, b_recv.at[t, 4 + 2 * kind])
        ref = region_ref(t, kind, *hi_pos[axis], 1)
        send(ref, ref, sent.at[4], b_recv.at[t, 7], lo_dev[axis])

    def first_own(t):
        arrived(staged.at[t], b_recv.at[t, 0])
        for kind in range(2):
            unit_own(t, kind)

    def first_relay(t):
        arrived(staged.at[t], b_recv.at[t, 1])
        for kind in range(2):
            unit_relay(t, kind)

    def second_own(t):
        arrived(staged.at[0:2], b_recv.at[t, 2])
        for kind in range(2):
            region_own(t, kind)

    def second_relay(t):
        for kind in range(2):
            region_relay(t, kind)

    def product(t, sp):
        s, h = t // 2, t % 2
        lhs = l_all[s, sp * BLOCK:(sp + 1) * BLOCK, :]
        for n in range(2):
            rhs = b_all[t, :, :, :, :, n * 256:(n + 1) * 256].reshape(1024, 256)
            p = jnp.dot(lhs, rhs, preferred_element_type=F32)
            for j in range(2):
                part = p[:, j * HALF:(j + 1) * HALF]
                if s > 0:
                    part = part + acc[sp, h, 2 * n + j]
                acc[sp, h, 2 * n + j] = part

    def compute(t):
        s = t // 2
        arrived(b_all.at[t, 0], b_recv.at[t, 7])
        if t % 2 == 0:
            arrived(l_all.at[s, pl.ds(s * BLOCK, 1024 - s * BLOCK), :], l_recv.at[s])
        product(t, s)

    def part_ref(t, slot, half):
        return acc.at[t // 2, t % 2, slot, pl.ds(half * HALF, HALF), :]

    xp1, xm1, xp2 = _rem4(x + 1), _rem4(x - 1), _rem4(x + 2)

    def reduce_first(t):
        send(part_ref(t, xp2, 0), relay_lo.at[t], sent.at[5], r_recv.at[t, 0], x_hi)
        send(part_ref(t, xp2, 1), relay_hi.at[t], sent.at[5], r_recv.at[t, 1], x_lo)
        send(part_ref(t, xp1, 1), from_lo.at[t, pl.ds(HALF, HALF), :], sent.at[5], r_recv.at[t, 2], x_hi)
        send(part_ref(t, xm1, 0), from_hi.at[t, pl.ds(0, HALF), :], sent.at[5], r_recv.at[t, 2], x_lo)

    def reduce_second(t):
        s, h = t // 2, t % 2
        arrived(relay_lo.at[t], r_recv.at[t, 0])
        acc[s, h, xp1, 0:HALF, :] = acc[s, h, xp1, 0:HALF, :] + relay_lo[t]
        send(part_ref(t, xp1, 0), from_lo.at[t, pl.ds(0, HALF), :], sent.at[5], r_recv.at[t, 2], x_hi)
        arrived(relay_hi.at[t], r_recv.at[t, 1])
        acc[s, h, xm1, HALF:BLOCK, :] = acc[s, h, xm1, HALF:BLOCK, :] + relay_hi[t]
        send(part_ref(t, xm1, 1), from_hi.at[t, pl.ds(HALF, HALF), :], sent.at[5], r_recv.at[t, 2], x_lo)

    def finish(t):
        s, h = t // 2, t % 2
        arrived(from_lo.at[0:2], r_recv.at[t, 2])
        total = acc[s, h, x] + from_lo[t] + from_hi[t]
        out_ref[s * BLOCK:(s + 1) * BLOCK, h * HALF:(h + 1) * HALF] = total.astype(out_ref.dtype)

    def others(t):
        for sp in range(t // 2 + 1, SLABS):
            product(t, sp)

    steps = {"move": move, "enter": enter, "own1": first_own, "relay1": first_relay, "own2": second_own, "relay2": second_relay,
             "compute": compute, "reduce1": reduce_first, "others": others, "reduce2": reduce_second, "finish": finish}
    for i in range(-4, STAGES + 8):
        for name, lag in ORDER:
            t = i - lag
            if 0 <= t < STAGES and not (name == "move" and t < MOVE_FIRST):
                steps[name](t)

    arrived(l_all.at[:, 0:320, :], sent.at[0])
    for i, few in ((1, jnp.logical_or(x == 0, x == 3)), (2, jnp.logical_or(plane_of(z, y) == 0, plane_of(z, y) == 3))):
        @pl.when(few)
        def _():
            arrived(staged.at[0:4], sent.at[i])

        @pl.when(jnp.logical_not(few))
        def _():
            arrived(staged, sent.at[i])
    arrived(l_all.at[0, 0:768, :], sent.at[3])
    arrived(b_all.at[0:6], sent.at[4])
    arrived(l_all.at[0:3, 0:512, :], sent.at[5])


def solution(mesh):
    def local_product(lower_loc, rhs_loc):
        rows, cols = rhs_loc.shape
        bf16 = lower_loc.dtype
        return pl.pallas_call(
            _kernel,
            out_shape=jax.ShapeDtypeStruct((rows, cols), bf16),
            in_specs=[pl.BlockSpec(memory_space=pltpu.HBM)] * 2,
            out_specs=pl.BlockSpec(memory_space=pltpu.VMEM),
            scratch_shapes=[
                pltpu.VMEM((SLABS, 1024, 1024), bf16),
                pltpu.VMEM((STAGES, 2, 2, 2, HALF, 512), bf16),
                pltpu.VMEM((SLABS, 2, 4, BLOCK, HALF), F32),
                pltpu.VMEM((STAGES, HALF, HALF), F32),
                pltpu.VMEM((STAGES, HALF, HALF), F32),
                pltpu.VMEM((STAGES, BLOCK, HALF), F32),
                pltpu.VMEM((STAGES, BLOCK, HALF), F32),
                pltpu.VMEM((STAGES, 2, HALF, HALF), bf16),
                pltpu.SemaphoreType.DMA((SLABS,)),
                pltpu.SemaphoreType.DMA((STAGES, 2)),
                pltpu.SemaphoreType.DMA((STAGES, 8)),
                pltpu.SemaphoreType.DMA((STAGES, 3)),
                pltpu.SemaphoreType.DMA((6,)),
            ],
            compiler_params=pltpu.CompilerParams(collective_id=0, has_side_effects=True, vmem_limit_bytes=63 * 1024 * 1024),
        )(lower_loc, rhs_loc)

    return jax.shard_map(local_product, mesh=mesh, in_specs=(P("row", "col"), P("row", ("batch", "col"))), out_specs=P("row", ("batch", "col")), check_vma=False)
```

```python
import jax
import jax.numpy as jnp
from jax import lax
from jax.experimental import pallas as pl
from jax.experimental.pallas import tpu as pltpu
from jax.sharding import PartitionSpec as P

BLOCK = 256
HALF = 128
STAGES = 8
SLABS = 4
MESH = pl.DeviceIdType.MESH
F32 = jnp.float32
MASKS = (0, 3, 1, 2, 0, 3, 1, 2)
AHEAD = (3, 4, 2)
DIRECT = 1
ROUND = (("relay2", 0), ("own2", 2), ("compute", -1), ("reduce1", -1), ("reduce2", -2), ("others", -1), ("finish", -4))


def _program_order():
    first, names = [], ("enter", "own1", "relay1")
    for i in range(5 * STAGES):
        lag = 0
        for k, name in enumerate(names):
            if 0 <= i - lag < STAGES:
                first.append((name, i - lag))
            lag += AHEAD[k]
        for t in range(2):
            if i == lag + t:
                first.append(("own2", t))
    second = [(name, i + d) for i in range(-2, STAGES + 6) for name, d in ROUND
              if 0 <= i + d < STAGES and not (name == "own2" and i + d < 2)]
    return first + second


def _rem4(v):
    return lax.rem(v + 8, 4)


def _kernel(l_hbm, b_hbm, out_ref, l_all, b_all, acc, relay_lo, relay_hi, from_lo, from_hi,
            staged, b_home, l_recv, m_recv, b_recv, r_recv, sent, home_sem, out_buf):
    row = lax.axis_index("row")
    col = lax.axis_index("col")
    z, y = row // 4, lax.rem(row, 4)
    x, core = col // 2, lax.rem(col, 2)

    def dev(zz, yy, xx, cc=None):
        return {"row": zz * 4 + yy, "col": xx * 2 + (core if cc is None else cc)}

    z_lo, z_hi = dev(_rem4(z - 1), y, x), dev(_rem4(z + 1), y, x)
    y_lo, y_hi = dev(z, _rem4(y - 1), x), dev(z, _rem4(y + 1), x)
    x_lo, x_hi = dev(z, y, _rem4(x - 1)), dev(z, y, _rem4(x + 1))
    partner = dev(z, y, x, 1 - core)

    def mix(t, v):
        m = MASKS[t]
        v = v if m % 2 == 0 else v + 1 - 2 * lax.rem(v, 2)
        return v if m < 2 else lax.rem(v + 2, 4)

    def offsets(kind, t, xs):
        v = mix(t, xs)
        hi, lo = v // 2, lax.rem(v, 2)
        return (hi, lo) if kind == 0 else (lo, hi)

    def moved(kind, back, zz, yy, off_z, off_y):
        dz = off_z if (kind == 0) != back else -off_z
        return _rem4(zz + dz), _rem4(yy + (2 * lax.rem(yy, 2) - 1) * off_y)

    def plane_of(zz, yy):
        return 2 * lax.rem(zz, 2) + yy // 2

    def root_info(kind, zt, yt):
        dz = _rem4(zt - x // 2)
        dy = _rem4(yt - 2 * lax.rem(x, 2) + 1)
        off_z = lax.rem(dz, 2)
        blk = dz // 2 if kind == 0 else lax.rem((dz + 1) // 2, 2)
        par, off_y = dy // 2, 1 - lax.rem((dy + 1) // 2, 2)
        return off_z, blk, par, off_y

    def slab_copy(s):
        rows = pl.ds(s * BLOCK, 1024 - s * BLOCK)
        return l_hbm.at[rows, pl.ds(s * 512, 512)], l_all.at[s, rows, pl.ds(pl.multiple_of(core * 512, 512), 512)]

    home_copy = pltpu.make_async_copy(b_hbm, b_home, home_sem)
    home_copy.start()
    for s in range(SLABS):
        src, dst = slab_copy(s)
        pltpu.make_async_copy(src, dst, l_recv.at[s]).start()

    barrier = pltpu.get_barrier_semaphore()
    y_far, z_far = dev(z, _rem4(y + 2), x), dev(_rem4(z + 2), y, x)
    y_side = _rem4(y + 2 * lax.rem(y, 2) - 1)
    for d in (z_lo, z_hi, y_lo, y_hi, x_lo, x_hi, dev(z, y, _rem4(x + 2)), partner, y_far, z_far,
              dev(_rem4(z - 1), y_side, x), dev(_rem4(z + 1), y_side, x)):
        pl.semaphore_signal(barrier, inc=1, device_id=d, device_id_type=MESH)
    home_copy.wait()
    pl.semaphore_wait(barrier, 12)

    def send(src, dst, s_sem, r_sem, where):
        cp = pltpu.make_async_remote_copy(src_ref=src, dst_ref=dst, send_sem=s_sem, recv_sem=r_sem,
                                          device_id=where, device_id_type=MESH)
        cp.start()

    def arrived(ref, sem):
        pltpu.make_async_copy(ref, ref, sem).wait()

    in_plane = plane_of(z, y) == x

    def final_ref(t, kind, zs, ys, xs):
        return b_all.at[t, lax.rem(ys, 2), zs // 2, kind, :, pl.ds(pl.multiple_of(xs * HALF, HALF), HALF)]

    def move_copies(t, kind):
        s, h = t // 2, t % 2
        here = (pl.ds(s * BLOCK + kind * HALF, HALF), pl.ds(h * HALF, HALF))
        off_z, off_y = offsets(kind, t, x)
        zt, yt = moved(kind, False, z, y, off_z, off_y)
        stay = x == MASKS[t]
        for direct in (True, False):
            dst = final_ref(t, kind, z, y, x) if direct else staged.at[t, kind]
            sem = b_recv.at[t, 0] if direct else m_recv.at[t, kind]
            cond = in_plane if direct else jnp.logical_not(in_plane)
            yield (jnp.logical_and(cond, stay), pltpu.make_async_copy(b_hbm.at[here], dst, sem), False)
            yield (jnp.logical_and(cond, jnp.logical_not(stay)),
                   pltpu.make_async_remote_copy(src_ref=b_home.at[here], dst_ref=dst, send_sem=sent.at[1], recv_sem=sem,
                                                device_id=dev(zt, yt, x), device_id_type=MESH), True)

    def move(t):
        for kind in range(2):
            for cond, cp, _ in move_copies(t, kind):
                pl.when(cond)(cp.start)

    def enter_copy(t, kind):
        off_z, off_y = offsets(kind, t, x)
        zs, ys = moved(kind, True, z, y, off_z, off_y)
        xt = plane_of(zs, ys)
        cp = pltpu.make_async_remote_copy(src_ref=staged.at[t, kind], dst_ref=final_ref(t, kind, zs, ys, x),
                                          send_sem=sent.at[2], recv_sem=b_recv.at[t, 0],
                                          device_id=dev(z, y, xt), device_id_type=MESH)
        return xt != x, cp

    def enter(t):
        for kind in range(2):
            cond, cp = enter_copy(t, kind)

            @pl.when(cond)
            def _():
                arrived(staged.at[t, kind], m_recv.at[t, kind])
                cp.start()

    for t in range(STAGES):
        move(t)

    for s in range(SLABS):
        src, dst = slab_copy(s)
        send(src, dst, sent.at[0], l_recv.at[s], partner)

    def unit_ref(t, kind, zt, yt):
        off_z, blk, par, off_y = root_info(kind, zt, yt)
        v = 2 * off_z + off_y if kind == 0 else 2 * off_y + off_z
        xs = mix(t, v)
        return b_all.at[t, par, blk, kind, :, pl.ds(pl.multiple_of(xs * HALF, HALF), HALF)]

    def region_ref(t, kind, zt, yt, half):
        off_z, blk, par, off_y = root_info(kind, zt, yt)
        pair = off_z if kind == 0 else off_y
        cols = pl.ds(pl.multiple_of((pair if MASKS[t] < 2 else 1 - pair) * 256, 256), 256)
        if kind == 0:
            return b_all.at[t, half, blk, 0, :, cols]
        return b_all.at[t, par, half, 1, :, cols]

    lo_pos = [(z, _rem4(y - 1)), (_rem4(z - 1), y)]
    hi_pos = [(z, _rem4(y + 1)), (_rem4(z + 1), y)]
    lo_dev, hi_dev, far_dev = [y_lo, z_lo], [y_hi, z_hi], [y_far, z_far]
    any_unit = b_all.at[0, 0, 0, 0, :, pl.ds(0, HALF)]
    any_region = b_all.at[0, 0, 0, 0, :, pl.ds(0, 256)]

    def unit_own(t, kind):
        ref, up = unit_ref(t, kind, z, y), (t + kind) % 2 == 0
        if t < DIRECT:
            for d in (hi_dev[kind], lo_dev[kind], far_dev[kind]):
                send(ref, ref, sent.at[3], b_recv.at[t, 2], d)
            return
        send(ref, ref, sent.at[3], b_recv.at[t, 1 if up else 2], hi_dev[kind])
        send(ref, ref, sent.at[3], b_recv.at[t, 2 if up else 1], lo_dev[kind])

    def unit_relay(t, kind):
        up = (t + kind) % 2 == 0
        ref = unit_ref(t, kind, *(lo_pos if up else hi_pos)[kind])
        send(ref, ref, sent.at[3], b_recv.at[t, 2], (hi_dev if up else lo_dev)[kind])

    def region_own(t, kind):
        axis = 1 - kind
        for j in range(2):
            up, down = region_ref(t, kind, z, y, j), region_ref(t, kind, z, y, 1 - j)
            send(up, up, sent.at[4], b_recv.at[t, 7 if j else 3 + 2 * kind], hi_dev[axis])
            send(down, down, sent.at[4], b_recv.at[t, 7 if j else 4 + 2 * kind], lo_dev[axis])

    def region_relay(t, kind):
        axis = 1 - kind
        arrived(any_region, b_recv.at[t, 3 + 2 * kind])
        ref = region_ref(t, kind, *lo_pos[axis], 0)
        send(ref, ref, sent.at[4], b_recv.at[t, 7], hi_dev[axis])
        arrived(any_region, b_recv.at[t, 4 + 2 * kind])
        ref = region_ref(t, kind, *hi_pos[axis], 1)
        send(ref, ref, sent.at[4], b_recv.at[t, 7], lo_dev[axis])

    def first_own(t):
        arrived(staged.at[t], b_recv.at[t, 0])
        for kind in range(2):
            unit_own(t, kind)

    def first_relay(t):
        if t < DIRECT:
            return
        arrived(staged.at[t], b_recv.at[t, 1])
        for kind in range(2):
            unit_relay(t, kind)

    def second_own(t):
        arrived(staged.at[0:3] if t < DIRECT else staged.at[0:2], b_recv.at[t, 2])
        for kind in range(2):
            region_own(t, kind)

    def second_relay(t):
        for kind in range(2):
            region_relay(t, kind)

    def product(t, sp):
        s, h = t // 2, t % 2
        lhs = l_all[s, sp * BLOCK:(sp + 1) * BLOCK, :]
        for n in range(2):
            rhs = b_all[t, :, :, :, :, n * 256:(n + 1) * 256].reshape(1024, 256)
            p = jnp.dot(lhs, rhs, preferred_element_type=F32)
            for j in range(2):
                part = p[:, j * HALF:(j + 1) * HALF]
                if s > 0:
                    part = part + acc[sp, h, 2 * n + j]
                acc[sp, h, 2 * n + j] = part

    def compute(t):
        s = t // 2
        arrived(b_all.at[t, 0], b_recv.at[t, 7])
        if t % 2 == 0:
            arrived(l_all.at[s, pl.ds(s * BLOCK, 1024 - s * BLOCK), :], l_recv.at[s])
        product(t, s)

    def part_ref(t, slot, half):
        return acc.at[t // 2, t % 2, slot, pl.ds(half * HALF, HALF), :]

    xp1, xm1, xp2 = _rem4(x + 1), _rem4(x - 1), _rem4(x + 2)

    def reduce_first(t):
        send(part_ref(t, xp2, 0), relay_lo.at[t], sent.at[5], r_recv.at[t, 0], x_hi)
        send(part_ref(t, xp2, 1), relay_hi.at[t], sent.at[5], r_recv.at[t, 1], x_lo)
        send(part_ref(t, xp1, 1), from_lo.at[t, pl.ds(HALF, HALF), :], sent.at[5], r_recv.at[t, 2], x_hi)
        send(part_ref(t, xm1, 0), from_hi.at[t, pl.ds(0, HALF), :], sent.at[5], r_recv.at[t, 2], x_lo)

    def reduce_second(t):
        s, h = t // 2, t % 2
        arrived(relay_lo.at[t], r_recv.at[t, 0])
        acc[s, h, xp1, 0:HALF, :] = acc[s, h, xp1, 0:HALF, :] + relay_lo[t]
        send(part_ref(t, xp1, 0), from_lo.at[t, pl.ds(0, HALF), :], sent.at[5], r_recv.at[t, 2], x_hi)
        arrived(relay_hi.at[t], r_recv.at[t, 1])
        acc[s, h, xm1, HALF:BLOCK, :] = acc[s, h, xm1, HALF:BLOCK, :] + relay_hi[t]
        send(part_ref(t, xm1, 1), from_hi.at[t, pl.ds(HALF, HALF), :], sent.at[5], r_recv.at[t, 2], x_lo)

    def finish(t):
        s, h = t // 2, t % 2
        arrived(from_lo.at[0:2], r_recv.at[t, 2])
        total = acc[s, h, x] + from_lo[t] + from_hi[t]
        out_buf[t] = total.astype(out_buf.dtype)
        pltpu.make_async_copy(out_buf.at[t], out_ref.at[pl.ds(s * BLOCK, BLOCK), pl.ds(h * HALF, HALF)], home_sem).start()

    def others(t):
        for sp in range(t // 2 + 1, SLABS):
            product(t, sp)

    steps = {"enter": enter, "own1": first_own, "relay1": first_relay, "own2": second_own, "relay2": second_relay,
             "compute": compute, "reduce1": reduce_first, "others": others, "reduce2": reduce_second, "finish": finish}
    for name, t in _program_order():
        steps[name](t)

    arrived(l_all.at[:, 0:320, :], sent.at[0])
    arrived(staged.at[0:6], sent.at[1])
    arrived(staged.at[0:6], sent.at[2])
    arrived(l_all.at[0, 0:768, :], sent.at[3])
    arrived(b_all.at[0:6], sent.at[4])
    arrived(l_all.at[0:3, 0:512, :], sent.at[5])
    arrived(out_buf, home_sem)


def solution(mesh):
    def local_product(lower_loc, rhs_loc):
        rows, cols = rhs_loc.shape
        bf16 = lower_loc.dtype
        return pl.pallas_call(
            _kernel,
            out_shape=jax.ShapeDtypeStruct((rows, cols), bf16),
            in_specs=[pl.BlockSpec(memory_space=pltpu.HBM)] * 2,
            out_specs=pl.BlockSpec(memory_space=pltpu.HBM),
            scratch_shapes=[
                pltpu.VMEM((SLABS, 1024, 1024), bf16),
                pltpu.VMEM((STAGES, 2, 2, 2, HALF, 512), bf16),
                pltpu.VMEM((SLABS, 2, 4, BLOCK, HALF), F32),
                pltpu.VMEM((STAGES, HALF, HALF), F32),
                pltpu.VMEM((STAGES, HALF, HALF), F32),
                pltpu.VMEM((STAGES, BLOCK, HALF), F32),
                pltpu.VMEM((STAGES, BLOCK, HALF), F32),
                pltpu.VMEM((STAGES, 2, HALF, HALF), bf16),
                pltpu.VMEM((rows, cols), bf16),
                pltpu.SemaphoreType.DMA((SLABS,)),
                pltpu.SemaphoreType.DMA((STAGES, 2)),
                pltpu.SemaphoreType.DMA((STAGES, 8)),
                pltpu.SemaphoreType.DMA((STAGES, 3)),
                pltpu.SemaphoreType.DMA((6,)),
                pltpu.SemaphoreType.DMA,
                pltpu.VMEM((STAGES, BLOCK, HALF), bf16),
            ],
            compiler_params=pltpu.CompilerParams(collective_id=0, has_side_effects=True, vmem_limit_bytes=63 * 1024 * 1024),
        )(lower_loc, rhs_loc)

    return jax.shard_map(local_product, mesh=mesh, in_specs=(P("row", "col"), P("row", ("batch", "col"))), out_specs=P("row", ("batch", "col")), check_vma=False)
```

```python
import jax
import jax.numpy as jnp
from jax import lax
from jax.experimental import pallas as pl
from jax.experimental.pallas import tpu as pltpu
from jax.sharding import PartitionSpec as P

BLOCK = 256
HALF = 128
STAGES = 8
SLABS = 4
MESH = pl.DeviceIdType.MESH
F32 = jnp.float32
MASKS = (2, 1, 0, 3, 2, 1, 0, 3)
AHEAD = (3, 4, 2)
DIRECT = 2
FINE, PIECES = 1, 2
ROUND = (("relay2", 0), ("own2", 2), ("compute", -1), ("reduce1", -1), ("reduce2", -2), ("others", -1), ("finish", -4))


def _program_order():
    first, names = [], ("enter", "own1", "relay1")
    for i in range(5 * STAGES):
        lag = 0
        for k, name in enumerate(names):
            if 0 <= i - lag < STAGES:
                first.append((name, i - lag))
            lag += AHEAD[k]
        for t in range(2):
            if i == lag + t:
                first.append(("own2", t))
    second = [(name, i + d) for i in range(-2, STAGES + 6) for name, d in ROUND
              if 0 <= i + d < STAGES and not (name == "own2" and i + d < 2)]
    return first + second


def _rem4(v):
    return lax.rem(v + 8, 4)


def _kernel(l_hbm, b_hbm, out_ref, l_all, b_all, acc, relay_lo, relay_hi, from_lo, from_hi,
            staged, b_home, l_recv, m_recv, b_recv, r_recv, sent, home_sem, out_buf, fine_recv):
    row = lax.axis_index("row")
    col = lax.axis_index("col")
    z, y = row // 4, lax.rem(row, 4)
    x, core = col // 2, lax.rem(col, 2)

    def dev(zz, yy, xx, cc=None):
        return {"row": zz * 4 + yy, "col": xx * 2 + (core if cc is None else cc)}

    z_lo, z_hi = dev(_rem4(z - 1), y, x), dev(_rem4(z + 1), y, x)
    y_lo, y_hi = dev(z, _rem4(y - 1), x), dev(z, _rem4(y + 1), x)
    x_lo, x_hi = dev(z, y, _rem4(x - 1)), dev(z, y, _rem4(x + 1))
    partner = dev(z, y, x, 1 - core)

    def mix(t, v):
        m = MASKS[t]
        v = v if m % 2 == 0 else v + 1 - 2 * lax.rem(v, 2)
        return v if m < 2 else lax.rem(v + 2, 4)

    def offsets(kind, t, xs):
        v = mix(t, xs)
        hi, lo = v // 2, lax.rem(v, 2)
        return (hi, lo) if kind == 0 else (lo, hi)

    def moved(kind, back, zz, yy, off_z, off_y):
        dz = off_z if (kind == 0) != back else -off_z
        return _rem4(zz + dz), _rem4(yy + (2 * lax.rem(yy, 2) - 1) * off_y)

    def plane_of(zz, yy):
        return 2 * lax.rem(zz, 2) + yy // 2

    def root_info(kind, zt, yt):
        dz = _rem4(zt - x // 2)
        dy = _rem4(yt - 2 * lax.rem(x, 2) + 1)
        off_z = lax.rem(dz, 2)
        blk = dz // 2 if kind == 0 else lax.rem((dz + 1) // 2, 2)
        par, off_y = dy // 2, 1 - lax.rem((dy + 1) // 2, 2)
        return off_z, blk, par, off_y

    def slab_copy(s):
        rows = pl.ds(s * BLOCK, 1024 - s * BLOCK)
        return l_hbm.at[rows, pl.ds(s * 512, 512)], l_all.at[s, rows, pl.ds(pl.multiple_of(core * 512, 512), 512)]

    home_copy = pltpu.make_async_copy(b_hbm, b_home, home_sem)
    home_copy.start()
    for s in range(SLABS):
        src, dst = slab_copy(s)
        pltpu.make_async_copy(src, dst, l_recv.at[s]).start()

    barrier = pltpu.get_barrier_semaphore()
    y_far, z_far = dev(z, _rem4(y + 2), x), dev(_rem4(z + 2), y, x)
    y_side = _rem4(y + 2 * lax.rem(y, 2) - 1)
    for d in (z_lo, z_hi, y_lo, y_hi, x_lo, x_hi, dev(z, y, _rem4(x + 2)), partner, y_far, z_far,
              dev(_rem4(z - 1), y_side, x), dev(_rem4(z + 1), y_side, x)):
        pl.semaphore_signal(barrier, inc=1, device_id=d, device_id_type=MESH)
    home_copy.wait()
    pl.semaphore_wait(barrier, 12)

    def send(src, dst, s_sem, r_sem, where):
        cp = pltpu.make_async_remote_copy(src_ref=src, dst_ref=dst, send_sem=s_sem, recv_sem=r_sem,
                                          device_id=where, device_id_type=MESH)
        cp.start()

    def arrived(ref, sem):
        pltpu.make_async_copy(ref, ref, sem).wait()

    in_plane = plane_of(z, y) == x

    def final_ref(t, kind, zs, ys, xs):
        return b_all.at[t, lax.rem(ys, 2), zs // 2, kind, :, pl.ds(pl.multiple_of(xs * HALF, HALF), HALF)]

    def move_copies(t, kind):
        s, h = t // 2, t % 2
        here = (pl.ds(s * BLOCK + kind * HALF, HALF), pl.ds(h * HALF, HALF))
        off_z, off_y = offsets(kind, t, x)
        zt, yt = moved(kind, False, z, y, off_z, off_y)
        stay = x == MASKS[t]
        for direct in (True, False):
            dst = final_ref(t, kind, z, y, x) if direct else staged.at[t, kind]
            sem = b_recv.at[t, 0] if direct else m_recv.at[t, kind]
            cond = in_plane if direct else jnp.logical_not(in_plane)
            yield (jnp.logical_and(cond, stay), pltpu.make_async_copy(b_hbm.at[here], dst, sem), False)
            yield (jnp.logical_and(cond, jnp.logical_not(stay)),
                   pltpu.make_async_remote_copy(src_ref=b_home.at[here], dst_ref=dst, send_sem=sent.at[1], recv_sem=sem,
                                                device_id=dev(zt, yt, x), device_id_type=MESH), True)

    def move(t):
        for kind in range(2):
            for cond, cp, _ in move_copies(t, kind):
                pl.when(cond)(cp.start)

    def enter_copy(t, kind):
        off_z, off_y = offsets(kind, t, x)
        zs, ys = moved(kind, True, z, y, off_z, off_y)
        xt = plane_of(zs, ys)
        cp = pltpu.make_async_remote_copy(src_ref=staged.at[t, kind], dst_ref=final_ref(t, kind, zs, ys, x),
                                          send_sem=sent.at[2], recv_sem=b_recv.at[t, 0],
                                          device_id=dev(z, y, xt), device_id_type=MESH)
        return xt != x, cp

    def enter(t):
        for kind in range(2):
            cond, cp = enter_copy(t, kind)

            @pl.when(cond)
            def _():
                arrived(staged.at[t, kind], m_recv.at[t, kind])
                cp.start()

    for t in range(STAGES):
        move(t)

    for s in range(SLABS):
        src, dst = slab_copy(s)
        send(src, dst, sent.at[0], l_recv.at[s], partner)

    def unit_ref(t, kind, zt, yt):
        off_z, blk, par, off_y = root_info(kind, zt, yt)
        v = 2 * off_z + off_y if kind == 0 else 2 * off_y + off_z
        xs = mix(t, v)
        return b_all.at[t, par, blk, kind, :, pl.ds(pl.multiple_of(xs * HALF, HALF), HALF)]

    def region_ref(t, kind, zt, yt, half):
        off_z, blk, par, off_y = root_info(kind, zt, yt)
        pair = off_z if kind == 0 else off_y
        cols = pl.ds(pl.multiple_of((pair if MASKS[t] < 2 else 1 - pair) * 256, 256), 256)
        if kind == 0:
            return b_all.at[t, half, blk, 0, :, cols]
        return b_all.at[t, par, half, 1, :, cols]

    lo_pos = [(z, _rem4(y - 1)), (_rem4(z - 1), y)]
    hi_pos = [(z, _rem4(y + 1)), (_rem4(z + 1), y)]
    lo_dev, hi_dev, far_dev = [y_lo, z_lo], [y_hi, z_hi], [y_far, z_far]
    any_unit = b_all.at[0, 0, 0, 0, :, pl.ds(0, HALF)]
    any_region = b_all.at[0, 0, 0, 0, :, pl.ds(0, 256)]

    def unit_own(t, kind):
        ref, up = unit_ref(t, kind, z, y), (t + kind) % 2 == 0
        if t < DIRECT:
            for d in (hi_dev[kind], lo_dev[kind], far_dev[kind]):
                send(ref, ref, sent.at[3], b_recv.at[t, 2], d)
            return
        send(ref, ref, sent.at[3], b_recv.at[t, 1 if up else 2], hi_dev[kind])
        send(ref, ref, sent.at[3], b_recv.at[t, 2 if up else 1], lo_dev[kind])

    def unit_relay(t, kind):
        up = (t + kind) % 2 == 0
        ref = unit_ref(t, kind, *(lo_pos if up else hi_pos)[kind])
        send(ref, ref, sent.at[3], b_recv.at[t, 2], (hi_dev if up else lo_dev)[kind])

    def region_own(t, kind):
        axis = 1 - kind
        for j in range(2):
            up, down = region_ref(t, kind, z, y, j), region_ref(t, kind, z, y, 1 - j)
            send(up, up, sent.at[4], b_recv.at[t, 7 if j else 3 + 2 * kind], hi_dev[axis])
            send(down, down, sent.at[4], b_recv.at[t, 7 if j else 4 + 2 * kind], lo_dev[axis])

    def region_relay(t, kind):
        axis = 1 - kind
        arrived(any_region, b_recv.at[t, 3 + 2 * kind])
        ref = region_ref(t, kind, *lo_pos[axis], 0)
        send(ref, ref, sent.at[4], b_recv.at[t, 7], hi_dev[axis])
        arrived(any_region, b_recv.at[t, 4 + 2 * kind])
        ref = region_ref(t, kind, *hi_pos[axis], 1)
        send(ref, ref, sent.at[4], b_recv.at[t, 7], lo_dev[axis])

    def first_own(t):
        arrived(staged.at[t], b_recv.at[t, 0])
        for kind in range(2):
            unit_own(t, kind)

    def first_relay(t):
        if t < DIRECT:
            return
        arrived(staged.at[t], b_recv.at[t, 1])
        for kind in range(2):
            unit_relay(t, kind)

    def second_own(t):
        arrived(staged.at[0:3] if t < DIRECT else staged.at[0:2], b_recv.at[t, 2])
        for kind in range(2):
            region_own(t, kind)

    def second_relay(t):
        for kind in range(2):
            region_relay(t, kind)

    xp1, xm1, xp2 = _rem4(x + 1), _rem4(x - 1), _rem4(x + 2)

    def product(t, sp, halves):
        s, h = t // 2, t % 2
        lhs = l_all[s, sp * BLOCK:(sp + 1) * BLOCK, :]
        for n in halves:
            cols = pl.ds(n * 256 if isinstance(n, int) else pl.multiple_of(n * 256, 256), 256)
            p = jnp.dot(lhs, b_all[t, :, :, :, :, cols].reshape(1024, 256), preferred_element_type=F32)
            for j in range(2):
                part = p[:, j * HALF:(j + 1) * HALF]
                if s > 0:
                    part = part + acc[sp, h, 2 * n + j]
                acc[sp, h, 2 * n + j] = part

    def compute(t):
        s = t // 2
        arrived(b_all.at[t, 0], b_recv.at[t, 7])
        if t % 2 == 0:
            arrived(l_all.at[s, pl.ds(s * BLOCK, 1024 - s * BLOCK), :], l_recv.at[s])
        product(t, s, [xp2 // 2])

    def part_ref(t, slot, half):
        return acc.at[t // 2, t % 2, slot, pl.ds(half * HALF, HALF), :]

    def pieces(t):
        n = PIECES if t >= STAGES - FINE else 1
        rows = HALF // n
        for q in range(n):
            sems = [fine_recv.at[t - STAGES + FINE, k, q] if n > 1 else r_recv.at[t, k] for k in range(2)]
            yield q * rows, rows, sems

    def reduce_first(t):
        s, h = t // 2, t % 2
        for r0, rows, sems in pieces(t):
            send(acc.at[s, h, xp2, pl.ds(r0, rows), :], relay_lo.at[t, pl.ds(r0, rows), :], sent.at[5], sems[0], x_hi)
            send(acc.at[s, h, xp2, pl.ds(HALF + r0, rows), :], relay_hi.at[t, pl.ds(r0, rows), :], sent.at[5], sems[1], x_lo)
        product(t, s, [1 - xp2 // 2])
        send(part_ref(t, xp1, 1), from_lo.at[t, pl.ds(HALF, HALF), :], sent.at[5], r_recv.at[t, 2], x_hi)
        send(part_ref(t, xm1, 0), from_hi.at[t, pl.ds(0, HALF), :], sent.at[5], r_recv.at[t, 2], x_lo)

    def reduce_second(t):
        s, h = t // 2, t % 2
        for r0, rows, sems in pieces(t):
            for sem, relay, slot, base, dst, to in ((sems[0], relay_lo, xp1, 0, from_lo, x_hi), (sems[1], relay_hi, xm1, HALF, from_hi, x_lo)):
                here = pl.ds(base + r0, rows)
                arrived(relay.at[t, pl.ds(r0, rows), :], sem)
                acc[s, h, slot, here, :] = acc[s, h, slot, here, :] + relay[t, pl.ds(r0, rows), :]
                send(acc.at[s, h, slot, here, :], dst.at[t, here, :], sent.at[5], r_recv.at[t, 2], to)

    def finish(t):
        s, h = t // 2, t % 2
        arrived(from_lo.at[0:2], r_recv.at[t, 2])
        total = acc[s, h, x] + from_lo[t] + from_hi[t]
        out_buf[t] = total.astype(out_buf.dtype)
        pltpu.make_async_copy(out_buf.at[t], out_ref.at[pl.ds(s * BLOCK, BLOCK), pl.ds(h * HALF, HALF)], home_sem).start()

    def others(t):
        for sp in range(t // 2 + 1, SLABS):
            product(t, sp, range(2))

    steps = {"enter": enter, "own1": first_own, "relay1": first_relay, "own2": second_own, "relay2": second_relay,
             "compute": compute, "reduce1": reduce_first, "others": others, "reduce2": reduce_second, "finish": finish}
    for name, t in _program_order():
        steps[name](t)

    arrived(l_all.at[:, 0:320, :], sent.at[0])
    arrived(staged.at[0:6], sent.at[1])
    arrived(staged.at[0:6], sent.at[2])
    arrived(l_all.at[0, 0:768, :], sent.at[3])
    arrived(b_all.at[0:6], sent.at[4])
    arrived(l_all.at[0:3, 0:512, :], sent.at[5])
    arrived(out_buf, home_sem)


def solution(mesh):
    def local_product(lower_loc, rhs_loc):
        rows, cols = rhs_loc.shape
        bf16 = lower_loc.dtype
        return pl.pallas_call(
            _kernel,
            out_shape=jax.ShapeDtypeStruct((rows, cols), bf16),
            in_specs=[pl.BlockSpec(memory_space=pltpu.HBM)] * 2,
            out_specs=pl.BlockSpec(memory_space=pltpu.HBM),
            scratch_shapes=[
                pltpu.VMEM((SLABS, 1024, 1024), bf16),
                pltpu.VMEM((STAGES, 2, 2, 2, HALF, 512), bf16),
                pltpu.VMEM((SLABS, 2, 4, BLOCK, HALF), F32),
                pltpu.VMEM((STAGES, HALF, HALF), F32),
                pltpu.VMEM((STAGES, HALF, HALF), F32),
                pltpu.VMEM((STAGES, BLOCK, HALF), F32),
                pltpu.VMEM((STAGES, BLOCK, HALF), F32),
                pltpu.VMEM((STAGES, 2, HALF, HALF), bf16),
                pltpu.VMEM((rows, cols), bf16),
                pltpu.SemaphoreType.DMA((SLABS,)),
                pltpu.SemaphoreType.DMA((STAGES, 2)),
                pltpu.SemaphoreType.DMA((STAGES, 8)),
                pltpu.SemaphoreType.DMA((STAGES, 3)),
                pltpu.SemaphoreType.DMA((6,)),
                pltpu.SemaphoreType.DMA,
                pltpu.VMEM((STAGES, BLOCK, HALF), bf16),
                pltpu.SemaphoreType.DMA((FINE, 2, PIECES)),
            ],
            compiler_params=pltpu.CompilerParams(collective_id=0, has_side_effects=True, vmem_limit_bytes=63 * 1024 * 1024),
        )(lower_loc, rhs_loc)

    return jax.shard_map(local_product, mesh=mesh, in_specs=(P("row", "col"), P("row", ("batch", "col"))), out_specs=P("row", ("batch", "col")), check_vma=False)
```

```python
import jax
import jax.numpy as jnp
from jax import lax
from jax.experimental import pallas as pl
from jax.experimental.pallas import tpu as pltpu
from jax.sharding import PartitionSpec as P

BLOCK = 256
HALF = 128
STAGES = 8
SLABS = 4
MESH = pl.DeviceIdType.MESH
F32 = jnp.float32
MASKS = (2, 1, 2, 1, 0, 3, 0, 3)
AHEAD = (3, 4, 2)
DIRECT = 2
FINE, PIECES = 1, 2
ROUND = (("relay2", 0), ("own2", 2), ("compute", -1), ("reduce1", -1), ("reduce2", -2), ("others", -1), ("finish", -4))


def _program_order():
    first, names = [], ("enter", "own1", "relay1")
    for i in range(5 * STAGES):
        lag = 0
        for k, name in enumerate(names):
            if 0 <= i - lag < STAGES:
                first.append((name, i - lag))
            lag += AHEAD[k]
        for t in range(2):
            if i == lag + t:
                first.append(("own2", t))
    second = [(name, i + d) for i in range(-2, STAGES + 6) for name, d in ROUND
              if 0 <= i + d < STAGES and not (name == "own2" and i + d < 2)]
    return first + second


def _rem4(v):
    return lax.rem(v + 8, 4)


def _kernel(l_hbm, b_hbm, out_ref, l_all, b_all, acc, relay_lo, relay_hi, from_lo, from_hi,
            staged, b_home, l_recv, m_recv, b_recv, r_recv, sent, home_sem, out_buf, fine_recv):
    row = lax.axis_index("row")
    col = lax.axis_index("col")
    z, y = row // 4, lax.rem(row, 4)
    x, core = col // 2, lax.rem(col, 2)

    def dev(zz, yy, xx, cc=None):
        return {"row": zz * 4 + yy, "col": xx * 2 + (core if cc is None else cc)}

    z_lo, z_hi = dev(_rem4(z - 1), y, x), dev(_rem4(z + 1), y, x)
    y_lo, y_hi = dev(z, _rem4(y - 1), x), dev(z, _rem4(y + 1), x)
    x_lo, x_hi = dev(z, y, _rem4(x - 1)), dev(z, y, _rem4(x + 1))
    partner = dev(z, y, x, 1 - core)

    def mix(t, v):
        m = MASKS[t]
        v = v if m % 2 == 0 else v + 1 - 2 * lax.rem(v, 2)
        return v if m < 2 else lax.rem(v + 2, 4)

    def offsets(kind, t, xs):
        v = mix(t, xs)
        hi, lo = v // 2, lax.rem(v, 2)
        return (hi, lo) if kind == 0 else (lo, hi)

    def moved(kind, back, zz, yy, off_z, off_y):
        dz = off_z if (kind == 0) != back else -off_z
        return _rem4(zz + dz), _rem4(yy + (2 * lax.rem(yy, 2) - 1) * off_y)

    def plane_of(zz, yy):
        return 2 * lax.rem(zz, 2) + yy // 2

    def root_info(kind, zt, yt):
        dz = _rem4(zt - x // 2)
        dy = _rem4(yt - 2 * lax.rem(x, 2) + 1)
        off_z = lax.rem(dz, 2)
        blk = dz // 2 if kind == 0 else lax.rem((dz + 1) // 2, 2)
        par, off_y = dy // 2, 1 - lax.rem((dy + 1) // 2, 2)
        return off_z, blk, par, off_y

    def slab_copy(s):
        rows = pl.ds(s * BLOCK, 1024 - s * BLOCK)
        return l_hbm.at[rows, pl.ds(s * 512, 512)], l_all.at[s, rows, pl.ds(pl.multiple_of(core * 512, 512), 512)]

    home_copy = pltpu.make_async_copy(b_hbm, b_home, home_sem)
    home_copy.start()
    for s in range(SLABS):
        src, dst = slab_copy(s)
        pltpu.make_async_copy(src, dst, l_recv.at[s]).start()

    barrier = pltpu.get_barrier_semaphore()
    y_far, z_far = dev(z, _rem4(y + 2), x), dev(_rem4(z + 2), y, x)
    y_side = _rem4(y + 2 * lax.rem(y, 2) - 1)
    for d in (z_lo, z_hi, y_lo, y_hi, x_lo, x_hi, dev(z, y, _rem4(x + 2)), partner, y_far, z_far,
              dev(_rem4(z - 1), y_side, x), dev(_rem4(z + 1), y_side, x)):
        pl.semaphore_signal(barrier, inc=1, device_id=d, device_id_type=MESH)
    home_copy.wait()
    pl.semaphore_wait(barrier, 12)

    def send(src, dst, s_sem, r_sem, where):
        cp = pltpu.make_async_remote_copy(src_ref=src, dst_ref=dst, send_sem=s_sem, recv_sem=r_sem,
                                          device_id=where, device_id_type=MESH)
        cp.start()

    def arrived(ref, sem):
        pltpu.make_async_copy(ref, ref, sem).wait()

    in_plane = plane_of(z, y) == x

    def final_ref(t, kind, zs, ys, xs):
        return b_all.at[t, lax.rem(ys, 2), zs // 2, kind, :, pl.ds(pl.multiple_of(xs * HALF, HALF), HALF)]

    def move_copies(t, kind):
        s, h = t // 2, t % 2
        here = (pl.ds(s * BLOCK + kind * HALF, HALF), pl.ds(h * HALF, HALF))
        off_z, off_y = offsets(kind, t, x)
        zt, yt = moved(kind, False, z, y, off_z, off_y)
        stay = x == MASKS[t]
        for direct in (True, False):
            dst = final_ref(t, kind, z, y, x) if direct else staged.at[t, kind]
            sem = b_recv.at[t, 0] if direct else m_recv.at[t, kind]
            cond = in_plane if direct else jnp.logical_not(in_plane)
            yield (jnp.logical_and(cond, stay), pltpu.make_async_copy(b_hbm.at[here], dst, sem), False)
            yield (jnp.logical_and(cond, jnp.logical_not(stay)),
                   pltpu.make_async_remote_copy(src_ref=b_home.at[here], dst_ref=dst, send_sem=sent.at[1], recv_sem=sem,
                                                device_id=dev(zt, yt, x), device_id_type=MESH), True)

    def move(t):
        for kind in range(2):
            for cond, cp, _ in move_copies(t, kind):
                pl.when(cond)(cp.start)

    def enter_copy(t, kind):
        off_z, off_y = offsets(kind, t, x)
        zs, ys = moved(kind, True, z, y, off_z, off_y)
        xt = plane_of(zs, ys)
        cp = pltpu.make_async_remote_copy(src_ref=staged.at[t, kind], dst_ref=final_ref(t, kind, zs, ys, x),
                                          send_sem=sent.at[2], recv_sem=b_recv.at[t, 0],
                                          device_id=dev(z, y, xt), device_id_type=MESH)
        return xt != x, cp

    def enter(t):
        for kind in range(2):
            cond, cp = enter_copy(t, kind)

            @pl.when(cond)
            def _():
                arrived(staged.at[t, kind], m_recv.at[t, kind])
                cp.start()

    for t in range(STAGES):
        move(t)

    for s in range(SLABS):
        src, dst = slab_copy(s)
        send(src, dst, sent.at[0], l_recv.at[s], partner)

    def unit_ref(t, kind, zt, yt):
        off_z, blk, par, off_y = root_info(kind, zt, yt)
        v = 2 * off_z + off_y if kind == 0 else 2 * off_y + off_z
        xs = mix(t, v)
        return b_all.at[t, par, blk, kind, :, pl.ds(pl.multiple_of(xs * HALF, HALF), HALF)]

    def region_ref(t, kind, zt, yt, half):
        off_z, blk, par, off_y = root_info(kind, zt, yt)
        pair = off_z if kind == 0 else off_y
        cols = pl.ds(pl.multiple_of((pair if MASKS[t] < 2 else 1 - pair) * 256, 256), 256)
        if kind == 0:
            return b_all.at[t, half, blk, 0, :, cols]
        return b_all.at[t, par, half, 1, :, cols]

    lo_pos = [(z, _rem4(y - 1)), (_rem4(z - 1), y)]
    hi_pos = [(z, _rem4(y + 1)), (_rem4(z + 1), y)]
    lo_dev, hi_dev, far_dev = [y_lo, z_lo], [y_hi, z_hi], [y_far, z_far]
    any_unit = b_all.at[0, 0, 0, 0, :, pl.ds(0, HALF)]
    any_region = b_all.at[0, 0, 0, 0, :, pl.ds(0, 256)]

    def unit_own(t, kind):
        ref, up = unit_ref(t, kind, z, y), (t + kind) % 2 == 0
        if t < DIRECT:
            for d in (hi_dev[kind], lo_dev[kind], far_dev[kind]):
                send(ref, ref, sent.at[3], b_recv.at[t, 2], d)
            return
        send(ref, ref, sent.at[3], b_recv.at[t, 1 if up else 2], hi_dev[kind])
        send(ref, ref, sent.at[3], b_recv.at[t, 2 if up else 1], lo_dev[kind])

    def unit_relay(t, kind):
        up = (t + kind) % 2 == 0
        ref = unit_ref(t, kind, *(lo_pos if up else hi_pos)[kind])
        send(ref, ref, sent.at[3], b_recv.at[t, 2], (hi_dev if up else lo_dev)[kind])

    def region_own(t, kind):
        axis = 1 - kind
        for j in range(2):
            up, down = region_ref(t, kind, z, y, j), region_ref(t, kind, z, y, 1 - j)
            send(up, up, sent.at[4], b_recv.at[t, 7 if j else 3 + 2 * kind], hi_dev[axis])
            send(down, down, sent.at[4], b_recv.at[t, 7 if j else 4 + 2 * kind], lo_dev[axis])

    def region_relay(t, kind):
        axis = 1 - kind
        arrived(any_region, b_recv.at[t, 3 + 2 * kind])
        ref = region_ref(t, kind, *lo_pos[axis], 0)
        send(ref, ref, sent.at[4], b_recv.at[t, 7], hi_dev[axis])
        arrived(any_region, b_recv.at[t, 4 + 2 * kind])
        ref = region_ref(t, kind, *hi_pos[axis], 1)
        send(ref, ref, sent.at[4], b_recv.at[t, 7], lo_dev[axis])

    def first_own(t):
        arrived(staged.at[t], b_recv.at[t, 0])
        for kind in range(2):
            unit_own(t, kind)

    def first_relay(t):
        if t < DIRECT:
            return
        arrived(staged.at[t], b_recv.at[t, 1])
        for kind in range(2):
            unit_relay(t, kind)

    def second_own(t):
        arrived(staged.at[0:3] if t < DIRECT else staged.at[0:2], b_recv.at[t, 2])
        for kind in range(2):
            region_own(t, kind)

    def second_relay(t):
        for kind in range(2):
            region_relay(t, kind)

    xp1, xm1, xp2 = _rem4(x + 1), _rem4(x - 1), _rem4(x + 2)

    def product(t, sp, halves):
        s, h = t // 2, t % 2
        lhs = l_all[s, sp * BLOCK:(sp + 1) * BLOCK, :]
        for n in halves:
            cols = pl.ds(n * 256 if isinstance(n, int) else pl.multiple_of(n * 256, 256), 256)
            p = jnp.dot(lhs, b_all[t, :, :, :, :, cols].reshape(1024, 256), preferred_element_type=F32)
            for j in range(2):
                part = p[:, j * HALF:(j + 1) * HALF]
                if s > 0:
                    part = part + acc[sp, h, 2 * n + j]
                acc[sp, h, 2 * n + j] = part

    def compute(t):
        s = t // 2
        arrived(b_all.at[t, 0], b_recv.at[t, 7])
        if t % 2 == 0:
            arrived(l_all.at[s, pl.ds(s * BLOCK, 1024 - s * BLOCK), :], l_recv.at[s])
        product(t, s, [xp2 // 2])

    def part_ref(t, slot, half):
        return acc.at[t // 2, t % 2, slot, pl.ds(half * HALF, HALF), :]

    def pieces(t):
        n = PIECES if t >= STAGES - FINE else 1
        rows = HALF // n
        for q in range(n):
            sems = [fine_recv.at[t - STAGES + FINE, k, q] if n > 1 else r_recv.at[t, k] for k in range(2)]
            yield q * rows, rows, sems

    def reduce_first(t):
        s, h = t // 2, t % 2
        for r0, rows, sems in pieces(t):
            send(acc.at[s, h, xp2, pl.ds(r0, rows), :], relay_lo.at[t, pl.ds(r0, rows), :], sent.at[5], sems[0], x_hi)
            send(acc.at[s, h, xp2, pl.ds(HALF + r0, rows), :], relay_hi.at[t, pl.ds(r0, rows), :], sent.at[5], sems[1], x_lo)
        product(t, s, [1 - xp2 // 2])
        send(part_ref(t, xp1, 1), from_lo.at[t, pl.ds(HALF, HALF), :], sent.at[5], r_recv.at[t, 2], x_hi)
        send(part_ref(t, xm1, 0), from_hi.at[t, pl.ds(0, HALF), :], sent.at[5], r_recv.at[t, 2], x_lo)

    def reduce_second(t):
        s, h = t // 2, t % 2
        for r0, rows, sems in pieces(t):
            for sem, relay, slot, base, dst, to in ((sems[0], relay_lo, xp1, 0, from_lo, x_hi), (sems[1], relay_hi, xm1, HALF, from_hi, x_lo)):
                here = pl.ds(base + r0, rows)
                arrived(relay.at[t, pl.ds(r0, rows), :], sem)
                acc[s, h, slot, here, :] = acc[s, h, slot, here, :] + relay[t, pl.ds(r0, rows), :]
                send(acc.at[s, h, slot, here, :], dst.at[t, here, :], sent.at[5], r_recv.at[t, 2], to)

    def finish(t):
        s, h = t // 2, t % 2
        arrived(from_lo.at[0:2], r_recv.at[t, 2])
        total = acc[s, h, x] + from_lo[t] + from_hi[t]
        out_buf[t] = total.astype(out_buf.dtype)
        pltpu.make_async_copy(out_buf.at[t], out_ref.at[pl.ds(s * BLOCK, BLOCK), pl.ds(h * HALF, HALF)], home_sem).start()

    def others(t):
        for sp in range(t // 2 + 1, SLABS):
            product(t, sp, range(2))

    steps = {"enter": enter, "own1": first_own, "relay1": first_relay, "own2": second_own, "relay2": second_relay,
             "compute": compute, "reduce1": reduce_first, "others": others, "reduce2": reduce_second, "finish": finish}
    for name, t in _program_order():
        steps[name](t)

    arrived(l_all.at[:, 0:320, :], sent.at[0])
    arrived(staged.at[0:6], sent.at[1])
    arrived(staged.at[0:6], sent.at[2])
    arrived(l_all.at[0, 0:768, :], sent.at[3])
    arrived(b_all.at[0:6], sent.at[4])
    arrived(l_all.at[0:3, 0:512, :], sent.at[5])
    arrived(out_buf, home_sem)


def solution(mesh):
    def local_product(lower_loc, rhs_loc):
        rows, cols = rhs_loc.shape
        bf16 = lower_loc.dtype
        return pl.pallas_call(
            _kernel,
            out_shape=jax.ShapeDtypeStruct((rows, cols), bf16),
            in_specs=[pl.BlockSpec(memory_space=pltpu.HBM)] * 2,
            out_specs=pl.BlockSpec(memory_space=pltpu.HBM),
            scratch_shapes=[
                pltpu.VMEM((SLABS, 1024, 1024), bf16),
                pltpu.VMEM((STAGES, 2, 2, 2, HALF, 512), bf16),
                pltpu.VMEM((SLABS, 2, 4, BLOCK, HALF), F32),
                pltpu.VMEM((STAGES, HALF, HALF), F32),
                pltpu.VMEM((STAGES, HALF, HALF), F32),
                pltpu.VMEM((STAGES, BLOCK, HALF), F32),
                pltpu.VMEM((STAGES, BLOCK, HALF), F32),
                pltpu.VMEM((STAGES, 2, HALF, HALF), bf16),
                pltpu.VMEM((rows, cols), bf16),
                pltpu.SemaphoreType.DMA((SLABS,)),
                pltpu.SemaphoreType.DMA((STAGES, 2)),
                pltpu.SemaphoreType.DMA((STAGES, 8)),
                pltpu.SemaphoreType.DMA((STAGES, 3)),
                pltpu.SemaphoreType.DMA((6,)),
                pltpu.SemaphoreType.DMA,
                pltpu.VMEM((STAGES, BLOCK, HALF), bf16),
                pltpu.SemaphoreType.DMA((FINE, 2, PIECES)),
            ],
            compiler_params=pltpu.CompilerParams(collective_id=0, has_side_effects=True, vmem_limit_bytes=63 * 1024 * 1024),
        )(lower_loc, rhs_loc)

    return jax.shard_map(local_product, mesh=mesh, in_specs=(P("row", "col"), P("row", ("batch", "col"))), out_specs=P("row", ("batch", "col")), check_vma=False)
```

```python
import jax
import jax.numpy as jnp
from jax import lax
from jax.experimental import pallas as pl
from jax.experimental.pallas import tpu as pltpu
from jax.sharding import PartitionSpec as P

BLOCK = 256
HALF = 128
STAGES = 8
SLABS = 4
MESH = pl.DeviceIdType.MESH
F32 = jnp.float32
MASKS = (2, 2, 1, 1, 0, 3, 0, 3)
AHEAD = (3, 4, 2)
DIRECT = 2
FINE, PIECES = 1, 2
ROUND = (("relay2", 0), ("own2", 2), ("compute", -1), ("reduce1", -1), ("reduce2", -2), ("others", -1), ("finish", -4))


def _program_order():
    first, names = [], ("enter", "own1", "relay1")
    for i in range(5 * STAGES):
        lag = 0
        for k, name in enumerate(names):
            if 0 <= i - lag < STAGES:
                first.append((name, i - lag))
            lag += AHEAD[k]
        for t in range(2):
            if i == lag + t:
                first.append(("own2", t))
    second = [(name, i + d) for i in range(-2, STAGES + 6) for name, d in ROUND
              if 0 <= i + d < STAGES and not (name == "own2" and i + d < 2)]
    return first + second


def _rem4(v):
    return lax.rem(v + 8, 4)


def _kernel(l_hbm, b_hbm, out_ref, l_all, b_all, acc, relay_lo, relay_hi, from_lo, from_hi,
            staged, b_home, l_recv, m_recv, b_recv, r_recv, sent, home_sem, out_buf, fine_recv):
    row = lax.axis_index("row")
    col = lax.axis_index("col")
    z, y = row // 4, lax.rem(row, 4)
    x, core = col // 2, lax.rem(col, 2)

    def dev(zz, yy, xx, cc=None):
        return {"row": zz * 4 + yy, "col": xx * 2 + (core if cc is None else cc)}

    z_lo, z_hi = dev(_rem4(z - 1), y, x), dev(_rem4(z + 1), y, x)
    y_lo, y_hi = dev(z, _rem4(y - 1), x), dev(z, _rem4(y + 1), x)
    x_lo, x_hi = dev(z, y, _rem4(x - 1)), dev(z, y, _rem4(x + 1))
    partner = dev(z, y, x, 1 - core)

    def mix(t, v):
        m = MASKS[t]
        v = v if m % 2 == 0 else v + 1 - 2 * lax.rem(v, 2)
        return v if m < 2 else lax.rem(v + 2, 4)

    def offsets(kind, t, xs):
        v = mix(t, xs)
        hi, lo = v // 2, lax.rem(v, 2)
        return (hi, lo) if kind == 0 else (lo, hi)

    def moved(kind, back, zz, yy, off_z, off_y):
        dz = off_z if (kind == 0) != back else -off_z
        return _rem4(zz + dz), _rem4(yy + (2 * lax.rem(yy, 2) - 1) * off_y)

    def plane_of(zz, yy):
        return 2 * lax.rem(zz, 2) + yy // 2

    def root_info(kind, zt, yt):
        dz = _rem4(zt - x // 2)
        dy = _rem4(yt - 2 * lax.rem(x, 2) + 1)
        off_z = lax.rem(dz, 2)
        blk = dz // 2 if kind == 0 else lax.rem((dz + 1) // 2, 2)
        par, off_y = dy // 2, 1 - lax.rem((dy + 1) // 2, 2)
        return off_z, blk, par, off_y

    def slab_copy(s):
        rows = pl.ds(s * BLOCK, 1024 - s * BLOCK)
        return l_hbm.at[rows, pl.ds(s * 512, 512)], l_all.at[s, rows, pl.ds(pl.multiple_of(core * 512, 512), 512)]

    home_copy = pltpu.make_async_copy(b_hbm, b_home, home_sem)
    home_copy.start()
    for s in range(SLABS):
        src, dst = slab_copy(s)
        pltpu.make_async_copy(src, dst, l_recv.at[s]).start()

    barrier = pltpu.get_barrier_semaphore()
    y_far, z_far = dev(z, _rem4(y + 2), x), dev(_rem4(z + 2), y, x)
    y_side = _rem4(y + 2 * lax.rem(y, 2) - 1)
    for d in (z_lo, z_hi, y_lo, y_hi, x_lo, x_hi, dev(z, y, _rem4(x + 2)), partner, y_far, z_far,
              dev(_rem4(z - 1), y_side, x), dev(_rem4(z + 1), y_side, x)):
        pl.semaphore_signal(barrier, inc=1, device_id=d, device_id_type=MESH)
    home_copy.wait()
    pl.semaphore_wait(barrier, 12)

    def send(src, dst, s_sem, r_sem, where):
        cp = pltpu.make_async_remote_copy(src_ref=src, dst_ref=dst, send_sem=s_sem, recv_sem=r_sem,
                                          device_id=where, device_id_type=MESH)
        cp.start()

    def arrived(ref, sem):
        pltpu.make_async_copy(ref, ref, sem).wait()

    in_plane = plane_of(z, y) == x

    def final_ref(t, kind, zs, ys, xs):
        return b_all.at[t, lax.rem(ys, 2), zs // 2, kind, :, pl.ds(pl.multiple_of(xs * HALF, HALF), HALF)]

    def move_copies(t, kind):
        s, h = t // 2, t % 2
        here = (pl.ds(s * BLOCK + kind * HALF, HALF), pl.ds(h * HALF, HALF))
        off_z, off_y = offsets(kind, t, x)
        zt, yt = moved(kind, False, z, y, off_z, off_y)
        stay = x == MASKS[t]
        for direct in (True, False):
            dst = final_ref(t, kind, z, y, x) if direct else staged.at[t, kind]
            sem = b_recv.at[t, 0] if direct else m_recv.at[t, kind]
            cond = in_plane if direct else jnp.logical_not(in_plane)
            yield (jnp.logical_and(cond, stay), pltpu.make_async_copy(b_hbm.at[here], dst, sem), False)
            yield (jnp.logical_and(cond, jnp.logical_not(stay)),
                   pltpu.make_async_remote_copy(src_ref=b_home.at[here], dst_ref=dst, send_sem=sent.at[1], recv_sem=sem,
                                                device_id=dev(zt, yt, x), device_id_type=MESH), True)

    def move(t):
        for kind in range(2):
            for cond, cp, _ in move_copies(t, kind):
                pl.when(cond)(cp.start)

    def enter_copy(t, kind):
        off_z, off_y = offsets(kind, t, x)
        zs, ys = moved(kind, True, z, y, off_z, off_y)
        xt = plane_of(zs, ys)
        cp = pltpu.make_async_remote_copy(src_ref=staged.at[t, kind], dst_ref=final_ref(t, kind, zs, ys, x),
                                          send_sem=sent.at[2], recv_sem=b_recv.at[t, 0],
                                          device_id=dev(z, y, xt), device_id_type=MESH)
        return xt != x, cp

    def enter(t):
        for kind in range(2):
            cond, cp = enter_copy(t, kind)

            @pl.when(cond)
            def _():
                arrived(staged.at[t, kind], m_recv.at[t, kind])
                cp.start()

    for t in range(STAGES):
        move(t)

    for s in range(SLABS):
        src, dst = slab_copy(s)
        send(src, dst, sent.at[0], l_recv.at[s], partner)

    def unit_ref(t, kind, zt, yt):
        off_z, blk, par, off_y = root_info(kind, zt, yt)
        v = 2 * off_z + off_y if kind == 0 else 2 * off_y + off_z
        xs = mix(t, v)
        return b_all.at[t, par, blk, kind, :, pl.ds(pl.multiple_of(xs * HALF, HALF), HALF)]

    def region_ref(t, kind, zt, yt, half):
        off_z, blk, par, off_y = root_info(kind, zt, yt)
        pair = off_z if kind == 0 else off_y
        cols = pl.ds(pl.multiple_of((pair if MASKS[t] < 2 else 1 - pair) * 256, 256), 256)
        if kind == 0:
            return b_all.at[t, half, blk, 0, :, cols]
        return b_all.at[t, par, half, 1, :, cols]

    lo_pos = [(z, _rem4(y - 1)), (_rem4(z - 1), y)]
    hi_pos = [(z, _rem4(y + 1)), (_rem4(z + 1), y)]
    lo_dev, hi_dev, far_dev = [y_lo, z_lo], [y_hi, z_hi], [y_far, z_far]
    any_unit = b_all.at[0, 0, 0, 0, :, pl.ds(0, HALF)]
    any_region = b_all.at[0, 0, 0, 0, :, pl.ds(0, 256)]

    def unit_own(t, kind):
        ref, up = unit_ref(t, kind, z, y), (t + kind) % 2 == 0
        if t < DIRECT:
            for d in (hi_dev[kind], lo_dev[kind], far_dev[kind]):
                send(ref, ref, sent.at[3], b_recv.at[t, 2], d)
            return
        send(ref, ref, sent.at[3], b_recv.at[t, 1 if up else 2], hi_dev[kind])
        send(ref, ref, sent.at[3], b_recv.at[t, 2 if up else 1], lo_dev[kind])

    def unit_relay(t, kind):
        up = (t + kind) % 2 == 0
        ref = unit_ref(t, kind, *(lo_pos if up else hi_pos)[kind])
        send(ref, ref, sent.at[3], b_recv.at[t, 2], (hi_dev if up else lo_dev)[kind])

    def region_own(t, kind):
        axis = 1 - kind
        for j in range(2):
            up, down = region_ref(t, kind, z, y, j), region_ref(t, kind, z, y, 1 - j)
            send(up, up, sent.at[4], b_recv.at[t, 7 if j else 3 + 2 * kind], hi_dev[axis])
            send(down, down, sent.at[4], b_recv.at[t, 7 if j else 4 + 2 * kind], lo_dev[axis])

    def region_relay(t, kind):
        axis = 1 - kind
        arrived(any_region, b_recv.at[t, 3 + 2 * kind])
        ref = region_ref(t, kind, *lo_pos[axis], 0)
        send(ref, ref, sent.at[4], b_recv.at[t, 7], hi_dev[axis])
        arrived(any_region, b_recv.at[t, 4 + 2 * kind])
        ref = region_ref(t, kind, *hi_pos[axis], 1)
        send(ref, ref, sent.at[4], b_recv.at[t, 7], lo_dev[axis])

    def first_own(t):
        arrived(staged.at[t], b_recv.at[t, 0])
        for kind in range(2):
            unit_own(t, kind)

    def first_relay(t):
        if t < DIRECT:
            return
        arrived(staged.at[t], b_recv.at[t, 1])
        for kind in range(2):
            unit_relay(t, kind)

    def second_own(t):
        arrived(staged.at[0:3] if t < DIRECT else staged.at[0:2], b_recv.at[t, 2])
        for kind in range(2):
            region_own(t, kind)

    def second_relay(t):
        for kind in range(2):
            region_relay(t, kind)

    xp1, xm1, xp2 = _rem4(x + 1), _rem4(x - 1), _rem4(x + 2)

    def product(t, sp, halves):
        s, h = t // 2, t % 2
        lhs = l_all[s, sp * BLOCK:(sp + 1) * BLOCK, :]
        for n in halves:
            cols = pl.ds(n * 256 if isinstance(n, int) else pl.multiple_of(n * 256, 256), 256)
            p = jnp.dot(lhs, b_all[t, :, :, :, :, cols].reshape(1024, 256), preferred_element_type=F32)
            for j in range(2):
                part = p[:, j * HALF:(j + 1) * HALF]
                if s > 0:
                    part = part + acc[sp, h, 2 * n + j]
                acc[sp, h, 2 * n + j] = part

    def compute(t):
        s = t // 2
        arrived(b_all.at[t, 0], b_recv.at[t, 7])
        if t % 2 == 0:
            arrived(l_all.at[s, pl.ds(s * BLOCK, 1024 - s * BLOCK), :], l_recv.at[s])
        product(t, s, [xp2 // 2])

    def part_ref(t, slot, half):
        return acc.at[t // 2, t % 2, slot, pl.ds(half * HALF, HALF), :]

    def pieces(t):
        n = PIECES if t >= STAGES - FINE else 1
        rows = HALF // n
        for q in range(n):
            sems = [fine_recv.at[t - STAGES + FINE, k, q] if n > 1 else r_recv.at[t, k] for k in range(2)]
            yield q * rows, rows, sems

    def reduce_first(t):
        s, h = t // 2, t % 2
        for r0, rows, sems in pieces(t):
            send(acc.at[s, h, xp2, pl.ds(r0, rows), :], relay_lo.at[t, pl.ds(r0, rows), :], sent.at[5], sems[0], x_hi)
            send(acc.at[s, h, xp2, pl.ds(HALF + r0, rows), :], relay_hi.at[t, pl.ds(r0, rows), :], sent.at[5], sems[1], x_lo)
        product(t, s, [1 - xp2 // 2])
        send(part_ref(t, xp1, 1), from_lo.at[t, pl.ds(HALF, HALF), :], sent.at[5], r_recv.at[t, 2], x_hi)
        send(part_ref(t, xm1, 0), from_hi.at[t, pl.ds(0, HALF), :], sent.at[5], r_recv.at[t, 2], x_lo)

    def reduce_second(t):
        s, h = t // 2, t % 2
        for r0, rows, sems in pieces(t):
            for sem, relay, slot, base, dst, to in ((sems[0], relay_lo, xp1, 0, from_lo, x_hi), (sems[1], relay_hi, xm1, HALF, from_hi, x_lo)):
                here = pl.ds(base + r0, rows)
                arrived(relay.at[t, pl.ds(r0, rows), :], sem)
                acc[s, h, slot, here, :] = acc[s, h, slot, here, :] + relay[t, pl.ds(r0, rows), :]
                send(acc.at[s, h, slot, here, :], dst.at[t, here, :], sent.at[5], r_recv.at[t, 2], to)

    def finish(t):
        s, h = t // 2, t % 2
        arrived(from_lo.at[0:2], r_recv.at[t, 2])
        total = acc[s, h, x] + from_lo[t] + from_hi[t]
        out_buf[t] = total.astype(out_buf.dtype)
        pltpu.make_async_copy(out_buf.at[t], out_ref.at[pl.ds(s * BLOCK, BLOCK), pl.ds(h * HALF, HALF)], home_sem).start()

    def others(t):
        for sp in range(t // 2 + 1, SLABS):
            product(t, sp, range(2))

    steps = {"enter": enter, "own1": first_own, "relay1": first_relay, "own2": second_own, "relay2": second_relay,
             "compute": compute, "reduce1": reduce_first, "others": others, "reduce2": reduce_second, "finish": finish}
    for name, t in _program_order():
        steps[name](t)

    arrived(l_all.at[:, 0:320, :], sent.at[0])
    arrived(staged.at[0:6], sent.at[1])
    arrived(staged.at[0:6], sent.at[2])
    arrived(l_all.at[0, 0:768, :], sent.at[3])
    arrived(b_all.at[0:6], sent.at[4])
    arrived(l_all.at[0:3, 0:512, :], sent.at[5])
    arrived(out_buf, home_sem)


def solution(mesh):
    def local_product(lower_loc, rhs_loc):
        rows, cols = rhs_loc.shape
        bf16 = lower_loc.dtype
        return pl.pallas_call(
            _kernel,
            out_shape=jax.ShapeDtypeStruct((rows, cols), bf16),
            in_specs=[pl.BlockSpec(memory_space=pltpu.HBM)] * 2,
            out_specs=pl.BlockSpec(memory_space=pltpu.HBM),
            scratch_shapes=[
                pltpu.VMEM((SLABS, 1024, 1024), bf16),
                pltpu.VMEM((STAGES, 2, 2, 2, HALF, 512), bf16),
                pltpu.VMEM((SLABS, 2, 4, BLOCK, HALF), F32),
                pltpu.VMEM((STAGES, HALF, HALF), F32),
                pltpu.VMEM((STAGES, HALF, HALF), F32),
                pltpu.VMEM((STAGES, BLOCK, HALF), F32),
                pltpu.VMEM((STAGES, BLOCK, HALF), F32),
                pltpu.VMEM((STAGES, 2, HALF, HALF), bf16),
                pltpu.VMEM((rows, cols), bf16),
                pltpu.SemaphoreType.DMA((SLABS,)),
                pltpu.SemaphoreType.DMA((STAGES, 2)),
                pltpu.SemaphoreType.DMA((STAGES, 8)),
                pltpu.SemaphoreType.DMA((STAGES, 3)),
                pltpu.SemaphoreType.DMA((6,)),
                pltpu.SemaphoreType.DMA,
                pltpu.VMEM((STAGES, BLOCK, HALF), bf16),
                pltpu.SemaphoreType.DMA((FINE, 2, PIECES)),
            ],
            compiler_params=pltpu.CompilerParams(collective_id=0, has_side_effects=True, vmem_limit_bytes=63 * 1024 * 1024),
        )(lower_loc, rhs_loc)

    return jax.shard_map(local_product, mesh=mesh, in_specs=(P("row", "col"), P("row", ("batch", "col"))), out_specs=P("row", ("batch", "col")), check_vma=False)
```
